256 devices in a mesh: beam: 2 (over z), tm: 128 (over x, y, core).
Axes of the slice: x: 8, y: 8, z: 2, core: 2. Of those that a mesh axis runs over, the one named last changes fastest.
The devices are a block of a 8x8x16 slice.
Arguments:
- voltage: bfloat16 [2, 2, 16777216], P(None, None, ('beam', 'tm')), parts along dimension 2, may hold values from -11 to 11
- delays: int32 [64, 2048], replicated, may hold values from 0 to 96, as said below
- chan_mask: int32 [4096], P('beam'), parts along dimension 0, may hold values 0 or 1
Outputs:
- zscore: float32 [64, 8192], P(None, ('beam', 'tm')), parts along dimension 1
- trial_stats: float32 [3, 128], P(None, 'beam'), parts along dimension 1
The draws below stay inside these ranges and needn't reach their ends.
There are 2 independent parts, one for each index of `beam`. The reference program is written for one: setup_inputs(seed, part) draws one part's arguments, and reference() takes and returns one part's arrays. A program takes and returns all parts, laid end to end along the dimension named above; an argument that names none is the same for every part. Nothing has to cross between parts.
Inputs may be any that keep to these rules, and one draw needn't show every extreme that they name: For each trial the delays never rise from one channel to the next; the last channel's delays are 0, and the first channel's delay of some trial is 96.
All inputs are finite; a program needn't handle non-finite values.
Results may differ from the reference program's by a relative error of at most 0.002.
Values may be sent and summed in bfloat16 or wider, within the bound.
A program may use at most 64 MiB of HBM per device.

```python
import jax
import jax.numpy as jnp
from jax import lax

NCHAN = 2048
TAPS = 16
NDM = 64
SAMPLES = 8388608
MAXD = 96


def draw_voltage(key, part):
    noise_key = jax.random.fold_in(jax.random.fold_in(key, 11), 0)
    position = jnp.arange(SAMPLES, dtype=jnp.float32) / SAMPLES
    envelope = jnp.exp(0.5 * jnp.log(3.5) * position)
    values = jnp.clip(jax.random.normal(noise_key, (2, 2, SAMPLES), jnp.float32) * envelope, -11.0, 11.0)
    return values.astype(jnp.bfloat16)


def draw_delays(key, part):
    size_key, pick_key = jax.random.split(jax.random.fold_in(key, 23))
    reaches = jax.random.randint(size_key, (NDM,), 0, MAXD + 1)
    chosen = jax.random.randint(pick_key, (), 0, NDM)
    reaches = jnp.where(jnp.arange(NDM, dtype=jnp.int32) == chosen, MAXD, reaches)
    channel = jnp.arange(NCHAN, dtype=jnp.int32)
    scale_unit = max(1, (NCHAN - 1) * 3 * NCHAN // 4096)
    chan_curve = (NCHAN - 1 - channel) * (3 * NCHAN - channel) // scale_unit
    top_value = (NCHAN - 1) * 3 * NCHAN // scale_unit
    return (reaches[:, None] * chan_curve[None, :] // top_value).astype(jnp.int32)


def plant(array, rng, least, high):
    shape = array.shape
    place = [jax.random.randint(jax.random.fold_in(rng, axis), (), 0, shape[axis]) for axis in range(len(shape))]
    array = array.at[tuple(place)].set(least)
    longest = shape.index(max(shape))
    place[longest] = (place[longest] + 1) % shape[longest]
    return array.at[tuple(place)].set(high)


def setup_inputs(seed: int = 0, part: int = 0) -> dict:
    key_of = jax.random.split(jax.random.key(seed), 4)
    part_splits = jax.random.split(jax.random.fold_in(key_of[3], part), 4)
    return {
        "voltage": draw_voltage(jax.random.fold_in(jax.random.fold_in(key_of[3], part), 71), part),
        "delays": draw_delays(jax.random.fold_in(key_of[3], 71), part),
        "chan_mask": plant((jax.random.randint(part_splits[2], (NCHAN,), 0, 8) < 7).astype(jnp.int32), jax.random.fold_in(part_splits[2], 1), 0, 1),
    }


def prototype(tap_count, chan_count):
    length = tap_count * chan_count
    position = jnp.arange(length, dtype=jnp.float32)
    centred = (position - (length - 1) / 2.0) / chan_count
    window = 0.54 - 0.46 * jnp.cos(2.0 * jnp.pi * position / (length - 1))
    shaped = jnp.sinc(centred) * window
    shaped = shaped * jnp.sqrt(chan_count / jnp.sum(shaped * shaped))
    return shaped.reshape(tap_count, chan_count)

def dedisperse(padded, delays, out_width, block_rows):
    chan_count = padded.shape[0]
    offsets = jnp.arange(out_width, dtype=jnp.int32)

    def pick_row(row_values, row_delays):
        return row_values[row_delays[:, None] + offsets[None, :]]

    def add_block(block_index, running):
        first_row = (block_index * block_rows).astype(jnp.int32)
        rows_here = lax.dynamic_slice_in_dim(padded, first_row, block_rows, 0)
        delay_here = lax.dynamic_slice_in_dim(delays, first_row, block_rows, 1)
        picked = jax.vmap(pick_row)(rows_here, delay_here.T)
        return running + lax.optimization_barrier(jnp.sum(picked.astype(jnp.float32), axis=0))
    zero_sums = jnp.zeros((delays.shape[0], out_width), jnp.float32)
    return lax.fori_loop(0, chan_count // block_rows, add_block, zero_sums)

def reference(voltage, delays, chan_mask):
    frame_count = voltage.shape[2] // NCHAN
    framed = voltage.astype(jnp.float32).reshape(2, 2, frame_count, NCHAN)
    history = jnp.zeros((2, 2, TAPS - 1, NCHAN), jnp.float32)
    extended = jnp.concatenate([history, framed], axis=2)
    coeffs = prototype(TAPS, NCHAN)
    weighted = jnp.zeros((2, 2, frame_count, NCHAN), jnp.float32)
    for tap_index in range(TAPS):
        weighted = weighted + coeffs[tap_index] * extended[:, :, tap_index:tap_index + frame_count]
    spectra = jnp.fft.fft(lax.complex(weighted[:, 0], weighted[:, 1]), axis=-1) / jnp.sqrt(jnp.float32(NCHAN))
    energy = lax.optimization_barrier(jnp.sum(jnp.real(spectra) ** 2 + jnp.imag(spectra) ** 2, axis=0))
    detected = energy.T.astype(jnp.bfloat16)
    masked = detected * chan_mask.astype(jnp.bfloat16)[:, None]
    padded = jnp.concatenate([masked, jnp.zeros((NCHAN, MAXD), jnp.bfloat16)], axis=1)
    series = dedisperse(padded, delays, frame_count, 16)
    average = lax.optimization_barrier(jnp.sum(series, axis=1)) / frame_count
    peak_value = lax.optimization_barrier(jnp.max(series, axis=1))
    centred = series - average[:, None]
    variance = lax.optimization_barrier(jnp.sum(centred * centred, axis=1)) / frame_count
    deviation = jnp.sqrt(variance + 1e-05)
    zscore = centred / deviation[:, None]
    live_count = jnp.maximum(jnp.sum(chan_mask).astype(jnp.float32), 1.0)
    trial_stats = jnp.stack([average / live_count, deviation / live_count, (peak_value - average) / deviation])
    return (zscore, trial_stats)
```

```python
import functools

import jax
import jax.numpy as jnp
import numpy as np
from jax import lax
from jax.experimental import pallas as pl
from jax.experimental.pallas import tpu as pltpu
from jax.sharding import PartitionSpec as P

NCHAN = 2048
TAPS = 16
LOW = 16
HIGH = 128
BLOCK = 8
GROUP = 16
LANES = 128
DSPAN = 3
MESH = pl.DeviceIdType.MESH
F32 = jnp.float32
BF16 = jnp.bfloat16


def filter_table():
    length = TAPS * NCHAN
    position = np.arange(length, dtype=np.float64)
    centred = (position - (length - 1) / 2.0) / NCHAN
    window = 0.54 - 0.46 * np.cos(2.0 * np.pi * position / (length - 1))
    shaped = np.sinc(centred) * window
    shaped = shaped * np.sqrt(NCHAN / np.sum(shaped * shaped))
    rows = shaped.reshape(TAPS, LOW, 1, HIGH)
    return np.broadcast_to(rows, (TAPS, LOW, 2, HIGH)).reshape(TAPS, 2 * LOW, HIGH).astype(np.float32)


def split_table(table):
    high = table.astype(np.float32).astype(jnp.bfloat16)
    low = (table - high.astype(np.float64)).astype(np.float32).astype(jnp.bfloat16)
    return np.stack([high, low])


def first_table():
    angle = 2.0 * np.pi * (np.outer(np.arange(LOW), np.arange(LOW)) % LOW) / LOW
    turn = np.empty((2, LOW, LOW, 2))
    turn[0, :, :, 0] = np.cos(angle)
    turn[0, :, :, 1] = np.sin(angle)
    turn[1, :, :, 0] = -np.sin(angle)
    turn[1, :, :, 1] = np.cos(angle)
    full = np.zeros((2, LOW, BLOCK, BLOCK, LOW, 2))
    for frame in range(BLOCK):
        full[:, :, frame, frame] = turn
    side = 2 * LOW * BLOCK
    return split_table(full.reshape(side, side))


def twist_table():
    angle = 2.0 * np.pi * np.outer(np.arange(LOW), np.arange(HIGH)) / NCHAN
    both = np.stack([np.cos(angle), np.sin(angle)])
    return np.repeat(both, BLOCK, axis=1).astype(np.float32)


def second_table():
    angle = 2.0 * np.pi * (np.outer(np.arange(HIGH), np.arange(HIGH)) % HIGH) / HIGH
    top = np.concatenate([np.cos(angle), -np.sin(angle)], axis=1)
    bottom = np.concatenate([np.sin(angle), np.cos(angle)], axis=1)
    return split_table(np.concatenate([top, bottom], axis=0) / np.sqrt(NCHAN))


def dot(a, b):
    return jnp.dot(a, b, preferred_element_type=F32)


def kernel(
    tm_size, frames, trials,
    volt, delays, mask, coef, first, twist, second,
    zout, stats_out,
    x, c, b1, tw, b2, dl, mk, wh, wl, det, dt32, dtm, acc, part, parts_in, st_b, st_c, ser,
    load_sem, halo_send, halo_recv, part_send, part_recv, b_send, b_recv, c_send, c_recv,
):
    me = lax.axis_index("tm")
    hist = TAPS - 1
    rings = tm_size // GROUP
    row, col = me // GROUP, me % GROUP

    def peer(step):
        return lax.rem(me + step + tm_size, tm_size)

    def group_peer(step):
        return row * GROUP + lax.rem(col + step, GROUP)

    def ring_peer(step):
        return lax.rem(row + step, rings) * GROUP + col

    loads = [
        pltpu.make_async_copy(volt.at[p], x.at[p, pl.ds(hist, frames)], load_sem.at[p]) for p in range(2)
    ]
    for k, (source, target) in enumerate(
        [(coef, c), (first, b1), (twist, tw), (second, b2), (delays, dl), (mask, mk)]
    ):
        loads.append(pltpu.make_async_copy(source, target, load_sem.at[2 + k]))
    for load in loads:
        load.start()

    barrier = pltpu.get_barrier_semaphore()
    known = [peer(s) for k in range(1, DSPAN + 1) for s in (k, -k)]
    known += [group_peer(s) for s in range(1, GROUP)]
    known += [ring_peer(s) for s in range(1, rings)]
    for target in known:
        pl.semaphore_signal(barrier, inc=1, device_id={"tm": target}, device_id_type=MESH)
    loads[0].wait()
    loads[1].wait()
    pl.semaphore_wait(barrier, len(known))

    halos = []
    for p in range(2):
        halos.append(
            pltpu.make_async_remote_copy(
                src_ref=x.at[p, pl.ds(frames, hist)],
                dst_ref=x.at[p, pl.ds(0, hist)],
                send_sem=halo_send.at[p],
                recv_sem=halo_recv.at[p],
                device_id={"tm": peer(1)},
                device_id_type=MESH,
            )
        )
        halos[p].start()

    for load in loads[2:]:
        load.wait()

    def weigh(block):
        def step(k, carry):
            p, r = k // 2, k % 2
            rows = pl.ds(pl.multiple_of(r * 16, 16), 16)
            lanes = pl.ds(pl.multiple_of(p * LANES, LANES), LANES)
            sums = [None] * BLOCK
            for i in range(BLOCK + hist):
                value = x[p, block * BLOCK + i, rows, :].astype(F32)
                for f in range(BLOCK):
                    tap = i - f
                    if 0 <= tap < TAPS:
                        term = c[tap, rows, :] * value
                        sums[f] = term if tap == 0 else sums[f] + term
                        if tap == TAPS - 1:
                            high = sums[f].astype(BF16)
                            low = (sums[f] - high.astype(F32)).astype(BF16)
                            place = pl.ds(pl.multiple_of(f * 32 + r * 16, 16), 16)
                            wh[block, place, lanes] = high
                            wl[block, place, lanes] = low
            return carry

        lax.fori_loop(0, 4, step, 0)

    def transform(block):
        half = LOW * BLOCK
        z = dot(b1[0], wh[block]) + dot(b1[0], wl[block]) + dot(b1[1], wh[block])
        energy = None
        for p in range(2):
            zr = z[:half, p * LANES : (p + 1) * LANES]
            zi = z[half:, p * LANES : (p + 1) * LANES]
            turned = jnp.concatenate([zr * tw[0] + zi * tw[1], zi * tw[0] - zr * tw[1]], axis=1)
            high = turned.astype(BF16)
            low = (turned - high.astype(F32)).astype(BF16)
            u = dot(high, b2[0]) + dot(high, b2[1]) + dot(low, b2[0])
            power = u[:, :HIGH] * u[:, :HIGH] + u[:, HIGH:] * u[:, HIGH:]
            energy = power if p == 0 else energy + power
        for k in range(LOW):
            det[pl.ds(pl.multiple_of(block * BLOCK, BLOCK), BLOCK), k * HIGH : (k + 1) * HIGH] = energy[
                k * BLOCK : (k + 1) * BLOCK
            ]

    def blocks(begin, end):
        def step(block, carry):
            weigh(block)
            transform(block)
            return carry

        lax.fori_loop(begin, end, step, 0)

    blocks(2, 4)

    used = jnp.where(mk[...] > 0, dl[...], -1).astype(F32).astype(BF16)
    lane = lax.broadcasted_iota(jnp.int32, (trials, LANES), 1)
    trial = lax.broadcasted_iota(jnp.int32, (trials, LANES), 0)
    spread = (lax.rem(lane, trials) == trial).astype(F32).astype(BF16)
    dt32[...] = lax.dot_general(used, spread, (((0,), (0,)), ((), ())), preferred_element_type=F32)
    lane_k = lax.broadcasted_iota(jnp.int32, (HIGH, LANES), 1)
    offset = (lane_k // trials).astype(F32)
    for k in range(LOW):
        rows = dt32[pl.ds(k, HIGH, stride=LOW), :] - offset
        dtm[k * HIGH : (k + 1) * HIGH, :LANES] = rows.astype(BF16)
        dtm[k * HIGH : (k + 1) * HIGH, LANES:] = (rows - 2.0).astype(BF16)
    acc[...] = jnp.zeros_like(acc)

    for p in range(2):
        halos[p].wait_recv()

    @pl.when(me == 0)
    def _():
        x[:, :hist] = jnp.zeros((2, hist, 2 * LOW, HIGH), BF16)

    blocks(0, 2)

    span = DSPAN * frames
    chunk = 2 * HIGH

    def shift(a, carry):
        begin = pl.multiple_of(span - 8 * a, 8)
        for h in range(2):
            target = jnp.full((chunk, 2 * LANES), (8 * a + 4 * h).astype(F32)).astype(BF16)
            total = None
            for k in range(NCHAN // chunk):
                chosen = jnp.where(dtm[k * chunk : (k + 1) * chunk, :] == target, 1.0, 0.0).astype(BF16)
                term = dot(det[:, k * chunk : (k + 1) * chunk].astype(BF16), chosen)
                total = term if k == 0 else total + term
            acc[h, pl.ds(begin, frames), :] += total
        return carry

    lax.fori_loop(0, span // 8 + 1, shift, 0)

    even, odd = None, None
    rows_out = span + frames
    for h in range(2):
        for half in range(2):
            lanes = slice(half * LANES, (half + 1) * LANES)
            first_row = 4 * h + 2 * half
            left = acc[h, first_row : first_row + rows_out, lanes]
            right = acc[h, first_row + 1 : first_row + 1 + rows_out, lanes]
            even = left if even is None else even + left
            odd = right if odd is None else odd + right
    part[...] = even + pltpu.roll(odd, trials, 1)

    sends = []
    for k in range(1, DSPAN + 1):
        begin = span - k * frames
        copy = pltpu.make_async_remote_copy(
            src_ref=part.at[pl.ds(begin, frames)],
            dst_ref=parts_in.at[k - 1],
            send_sem=part_send.at[k - 1],
            recv_sem=part_recv.at[k - 1],
            device_id={"tm": peer(-k)},
            device_id_type=MESH,
        )
        copy.start()
        sends.append(copy)
    series = part[span:, :]
    for k in range(1, DSPAN + 1):
        sends[k - 1].wait_recv()
        inside = (me + k < tm_size).astype(F32)
        series = series + parts_in[k - 1] * inside

    def gather(slots, own, steps, to, send, recv):
        slots[0] = own
        copies = []
        for s in range(1, steps):
            copy = pltpu.make_async_remote_copy(
                src_ref=slots.at[0],
                dst_ref=slots.at[s],
                send_sem=send.at[s - 1],
                recv_sem=recv.at[s - 1],
                device_id={"tm": to(s)},
                device_id_type=MESH,
            )
            copy.start()
            copies.append(copy)
        for copy in copies:
            copy.wait_recv()
        return copies

    def pack(mean, second, peak):
        wide = lax.broadcasted_iota(jnp.int32, (1, LANES), 1)
        head = jnp.where(wide < trials, mean, pltpu.roll(second, trials, 1))
        return jnp.concatenate([head, peak], axis=0)

    def merge(slots, steps, count):
        heads = jnp.concatenate([slots[s, 0:1] for s in range(steps)], axis=0)
        peaks = jnp.concatenate([slots[s, 1:2] for s in range(steps)], axis=0)
        mean = jnp.sum(heads, axis=0, keepdims=True) / steps
        away = heads - mean
        seconds = pltpu.roll(mean * steps, trials, 1)
        second = seconds + count * jnp.sum(away * away, axis=0, keepdims=True)
        return mean, second, jnp.max(peaks, axis=0, keepdims=True)

    mean = jnp.sum(series, axis=0, keepdims=True) / frames
    away = series - mean
    second_sum = jnp.sum(away * away, axis=0, keepdims=True)
    peak = jnp.max(series, axis=0, keepdims=True)
    ser[...] = series
    b_copies = gather(st_b, pack(mean, second_sum, peak), GROUP, group_peer, b_send, b_recv)
    mean, second_sum, peak = merge(st_b, GROUP, float(frames))
    c_copies = gather(st_c, pack(mean, second_sum, peak), rings, ring_peer, c_send, c_recv)
    average, second_sum, peak = merge(st_c, rings, float(frames * GROUP))

    variance = second_sum / (frames * tm_size)
    deviation = jnp.sqrt(variance + 1e-05)
    z = (ser[...] - average) / deviation
    zout[...] = z[:, :trials]
    live = jnp.maximum(jnp.sum(mk[...].astype(F32)), 1.0)
    rows = jnp.concatenate([average / live, deviation / live, (peak - average) / deviation], axis=0)
    stats_out[...] = rows[:, :trials]

    for p in range(2):
        halos[p].wait_send()
    for copy in sends + b_copies + c_copies:
        copy.wait_send()


def per_device(tm_size, voltage, delays, chan_mask):
    frames = voltage.shape[2] // NCHAN
    trials = delays.shape[0]
    rows = voltage.shape[2] // HIGH
    volt = voltage.reshape(2, 2, rows, HIGH).transpose(0, 2, 1, 3).reshape(2, frames, 2 * LOW, HIGH)
    hist = TAPS - 1
    rings = tm_size // GROUP
    side = 2 * LOW * BLOCK
    vmem = pltpu.VMEM
    dma = pltpu.SemaphoreType.DMA
    span = DSPAN * frames
    zscore, stats = pl.pallas_call(
        functools.partial(kernel, tm_size, frames, trials),
        out_shape=(
            jax.ShapeDtypeStruct((frames, trials), F32),
            jax.ShapeDtypeStruct((3, trials), F32),
        ),
        in_specs=[pl.BlockSpec(memory_space=pl.ANY)] * 7,
        out_specs=(pl.BlockSpec(memory_space=pltpu.VMEM),) * 2,
        scratch_shapes=[
            vmem((2, hist + frames, 2 * LOW, HIGH), BF16),
            vmem((TAPS, 2 * LOW, HIGH), F32),
            vmem((2, side, side), BF16),
            vmem((2, LOW * BLOCK, HIGH), F32),
            vmem((2, 2 * HIGH, 2 * HIGH), BF16),
            vmem((trials, NCHAN), jnp.int32),
            vmem((1, NCHAN), jnp.int32),
            vmem((frames // BLOCK, side, 2 * LANES), BF16),
            vmem((frames // BLOCK, side, 2 * LANES), BF16),
            vmem((frames, NCHAN), F32),
            vmem((NCHAN, LANES), F32),
            vmem((NCHAN, 2 * LANES), BF16),
            vmem((2, span + frames + 8, 2 * LANES), F32),
            vmem((span + frames, LANES), F32),
            vmem((DSPAN, frames, LANES), F32),
            vmem((GROUP, 2, LANES), F32),
            vmem((rings, 2, LANES), F32),
            vmem((frames, LANES), F32),
            dma((8,)),
            dma((2,)),
            dma((2,)),
            dma((DSPAN,)),
            dma((DSPAN,)),
            dma((GROUP - 1,)),
            dma((GROUP - 1,)),
            dma((rings - 1,)),
            dma((rings - 1,)),
        ],
        compiler_params=pltpu.CompilerParams(
            collective_id=0, has_side_effects=True, vmem_limit_bytes=67043328
        ),
    )(
        volt, delays, chan_mask.reshape(1, NCHAN),
        jnp.asarray(filter_table()), jnp.asarray(first_table()),
        jnp.asarray(twist_table()), jnp.asarray(second_table()),
    )
    return zscore.T, stats


def solution(mesh):
    return jax.shard_map(
        functools.partial(per_device, mesh.shape["tm"]),
        mesh=mesh,
        in_specs=(P(None, None, ("beam", "tm")), P(), P("beam")),
        out_specs=(P(None, ("beam", "tm")), P(None, "beam")),
        check_vma=False,
    )
```

```python
import functools

import jax
import jax.numpy as jnp
import numpy as np
from jax import lax
from jax.experimental import pallas as pl
from jax.experimental.pallas import tpu as pltpu
from jax.sharding import PartitionSpec as P

NCHAN = 2048
TAPS = 16
LOW = 16
HIGH = 128
BLOCK = 8
GROUP = 16
LANES = 128
DSPAN = 3
CORES = 2
AHEAD = 4
MESH = pl.DeviceIdType.MESH
F32 = jnp.float32
BF16 = jnp.bfloat16


def filter_table():
    length = TAPS * NCHAN
    position = np.arange(length, dtype=np.float64)
    centred = (position - (length - 1) / 2.0) / NCHAN
    window = 0.54 - 0.46 * np.cos(2.0 * np.pi * position / (length - 1))
    shaped = np.sinc(centred) * window
    shaped = shaped * np.sqrt(NCHAN / np.sum(shaped * shaped))
    rows = shaped.reshape(TAPS, LOW, 1, HIGH)
    return np.broadcast_to(rows, (TAPS, LOW, 2, HIGH)).reshape(TAPS, 2 * LOW, HIGH).astype(np.float32)


def split_table(table):
    high = table.astype(np.float32).astype(jnp.bfloat16)
    low = (table - high.astype(np.float64)).astype(np.float32).astype(jnp.bfloat16)
    return np.stack([high, low])


def first_table():
    angle = 2.0 * np.pi * (np.outer(np.arange(LOW), np.arange(LOW)) % LOW) / LOW
    turn = np.empty((2, LOW, LOW, 2))
    turn[0, :, :, 0] = np.cos(angle)
    turn[0, :, :, 1] = np.sin(angle)
    turn[1, :, :, 0] = -np.sin(angle)
    turn[1, :, :, 1] = np.cos(angle)
    full = np.zeros((2, LOW, BLOCK, BLOCK, LOW, 2))
    for frame in range(BLOCK):
        full[:, :, frame, frame] = turn
    side = 2 * LOW * BLOCK
    return split_table(full.reshape(side, side))


def twist_table():
    angle = 2.0 * np.pi * np.outer(np.arange(LOW), np.arange(HIGH)) / NCHAN
    both = np.stack([np.cos(angle), np.sin(angle)])
    return np.repeat(both, BLOCK, axis=1).astype(np.float32)


def second_table():
    angle = 2.0 * np.pi * (np.outer(np.arange(HIGH), np.arange(HIGH)) % HIGH) / HIGH
    top = np.concatenate([np.cos(angle), -np.sin(angle)], axis=1)
    bottom = np.concatenate([np.sin(angle), np.cos(angle)], axis=1)
    return split_table(np.concatenate([top, bottom], axis=0) / np.sqrt(NCHAN))


def dot(a, b):
    return jnp.dot(a, b, preferred_element_type=F32)


def kernel(
    tm_size, frames, trials,
    volt, delays, mask, coef, first, twist, second,
    zout, stats_out,
    x, c, b1, tw, b2, dl, mk, wh, wl, det, dt32, dtm, acc, part, parts_in, st_a, st_b, st_c,
    load_sem, near_sem, past_sem, halo_send, halo_recv, part_send, part_recv, pair_send, pair_recv,
    b_send, b_recv, c_send, c_recv,
):
    me = lax.axis_index("tm")
    hist = TAPS - 1
    last = tm_size - 1
    rings = tm_size // GROUP
    side = GROUP // CORES
    core = lax.rem(me, CORES)
    place = me // CORES
    row, col = place // side, lax.rem(place, side)

    def signal(sem, target):
        pl.semaphore_signal(sem, inc=1, device_id={"tm": target}, device_id_type=MESH)

    def send(source, target, send_sem, recv_sem, device):
        return pltpu.make_async_remote_copy(
            src_ref=source, dst_ref=target, send_sem=send_sem, recv_sem=recv_sem,
            device_id={"tm": device}, device_id_type=MESH,
        )

    def col_peer(step):
        return (row * side + lax.rem(col + step, side)) * CORES + 1

    def row_peer(step, which):
        return (lax.rem(row + step, rings) * side + col) * CORES + which

    barrier = pltpu.get_barrier_semaphore()

    @pl.when(core == 1)
    def _():
        signal(barrier, me - 1)

        @pl.when(me < last)
        def _():
            signal(barrier, me + 1)

    loads = [
        pltpu.make_async_copy(volt.at[p], x.at[p, pl.ds(hist, frames)], load_sem.at[p]) for p in range(2)
    ]
    for k, (source, target) in enumerate(
        [(coef, c), (first, b1), (twist, tw), (second, b2), (delays, dl), (mask, mk)]
    ):
        loads.append(pltpu.make_async_copy(source, target, load_sem.at[2 + k]))
    for load in loads:
        load.start()

    @pl.when(core == 0)
    def _():
        pl.semaphore_wait(barrier, 1 + jnp.minimum(me, 1))
        signal(near_sem, me + 1)

        @pl.when(me > 0)
        def _():
            signal(near_sem, me - 1)

    def halo(k):
        p, rows = k // 2, pl.ds((k % 2) * 16, 16)
        return send(
            x.at[p, pl.ds(frames, hist), rows], x.at[p, pl.ds(0, hist), rows],
            halo_send.at[k], halo_recv.at[k], me + 1,
        )

    loads[0].wait()
    loads[1].wait()

    @pl.when(core == 1)
    def _():
        pl.semaphore_wait(near_sem, 1 + jnp.minimum(last - me, 1))

    @pl.when(me < last)
    def _():
        for k in range(4):
            halo(k).start()

    @pl.when(me == 0)
    def _():
        x[:, :hist] = jnp.zeros((2, hist, 2 * LOW, HIGH), BF16)

    @pl.when(core == 1)
    def _():
        for step in range(1, side):
            signal(barrier, col_peer(step))
        for step in range(1, rings):
            signal(barrier, row_peer(step, 1))

    for load in loads[2:]:
        load.wait()

    def weigh(block, k):
        p, r = k // 2, lax.rem(k, 2)
        rows = pl.ds(pl.multiple_of(r * 16, 16), 16)
        lanes = pl.ds(pl.multiple_of(p * LANES, LANES), LANES)
        sums = [None] * BLOCK
        for i in range(BLOCK + hist):
            value = x[p, block * BLOCK + i, rows, :].astype(F32)
            for f in range(BLOCK):
                tap = i - f
                if 0 <= tap < TAPS:
                    term = c[tap, rows, :] * value
                    sums[f] = term if tap == 0 else sums[f] + term
                    if tap == TAPS - 1:
                        high = sums[f].astype(BF16)
                        low = (sums[f] - high.astype(F32)).astype(BF16)
                        spot = pl.ds(pl.multiple_of(f * 32 + r * 16, 16), 16)
                        wh[block, spot, lanes] = high
                        wl[block, spot, lanes] = low

    def transform(pair):
        half = LOW * BLOCK
        energies = []
        turns = [
            dot(b1[0], wh[b]) + dot(b1[0], wl[b]) + dot(b1[1], wh[b]) for b in (2 * pair, 2 * pair + 1)
        ]
        for z in turns:
            energy = None
            for p in range(2):
                zr = z[:half, p * LANES : (p + 1) * LANES]
                zi = z[half:, p * LANES : (p + 1) * LANES]
                turned = jnp.concatenate([zr * tw[0] + zi * tw[1], zi * tw[0] - zr * tw[1]], axis=1)
                high = turned.astype(BF16)
                low = (turned - high.astype(F32)).astype(BF16)
                u = dot(high, b2[0]) + dot(high, b2[1]) + dot(low, b2[0])
                power = u[:, :HIGH] * u[:, :HIGH] + u[:, HIGH:] * u[:, HIGH:]
                energy = power if p == 0 else energy + power
            energies.append(energy)
        for k in range(LOW):
            both = jnp.concatenate([e[k * BLOCK : (k + 1) * BLOCK] for e in energies], axis=0)
            det[2 * pair * BLOCK : 2 * (pair + 1) * BLOCK, k * HIGH : (k + 1) * HIGH] = both.astype(BF16)

    def late_half(k, carry):
        weigh(2, k)
        weigh(3, k)
        return carry

    lax.fori_loop(0, 4, late_half, 0)
    transform(1)

    used = jnp.where(mk[...] > 0, dl[...], -1).astype(F32).astype(BF16)
    lane = lax.broadcasted_iota(jnp.int32, (trials, LANES), 1)
    trial = lax.broadcasted_iota(jnp.int32, (trials, LANES), 0)
    spread = (lax.rem(lane, trials) == trial).astype(F32).astype(BF16)
    dt32[...] = lax.dot_general(used, spread, (((0,), (0,)), ((), ())), preferred_element_type=F32)
    lane_k = lax.broadcasted_iota(jnp.int32, (HIGH, LANES), 1)
    offset = (lane_k // trials).astype(F32)
    for k in range(LOW):
        rows = dt32[pl.ds(k, HIGH, stride=LOW), :] - offset
        dtm[k * HIGH : (k + 1) * HIGH, :LANES] = rows.astype(BF16)
        dtm[k * HIGH : (k + 1) * HIGH, LANES:] = (rows - 2.0).astype(BF16)
    acc[...] = jnp.zeros_like(acc)

    for k in range(4):

        @pl.when(me > 0)
        def _():
            halo(k).wait_recv()

        def early_half(block, carry):
            weigh(block, k)
            return carry

        lax.fori_loop(0, 2, early_half, 0)

    @pl.when(core == 0)
    def _():
        signal(past_sem, me + 1)

    transform(0)

    span = DSPAN * frames
    chunk = 2 * HIGH

    def select(base, h):
        target = jnp.full((chunk, 2 * LANES), base + 4.0 * h).astype(BF16)
        total = None
        for k in range(NCHAN // chunk):
            chosen = jnp.where(dtm[k * chunk : (k + 1) * chunk, :] == target, 1.0, 0.0).astype(BF16)
            term = dot(det[:, k * chunk : (k + 1) * chunk], chosen)
            total = term if k == 0 else total + term
        return total

    def shift(i, carry):
        totals = []
        for j in range(AHEAD):
            a = i * AHEAD + j
            totals.append([select((8 * a).astype(F32), h) for h in range(2)])
        for j in range(AHEAD):
            begin = pl.multiple_of(span - 8 * (i * AHEAD + j), 8)
            for h in range(2):
                acc[h, pl.ds(begin, frames), :] += totals[j][h]
        return carry

    lax.fori_loop(0, span // 8 // AHEAD, shift, 0)
    acc[0, 0:frames, :] += select(float(span), 0)

    even, odd = None, None
    rows_out = span + frames
    for h in range(2):
        for half in range(2):
            lanes = slice(half * LANES, (half + 1) * LANES)
            first_row = 4 * h + 2 * half
            left = acc[h, first_row : first_row + rows_out, lanes]
            right = acc[h, first_row + 1 : first_row + 1 + rows_out, lanes]
            even = left if even is None else even + left
            odd = right if odd is None else odd + right
    part[...] = even + pltpu.roll(odd, trials, 1)

    @pl.when(core == 1)
    def _():
        pl.semaphore_wait(past_sem, 1)

    def part_copy(k):
        return send(
            part.at[pl.ds(span - k * frames, frames)], parts_in.at[k - 1],
            part_send.at[k - 1], part_recv.at[k - 1], me - k,
        )

    for k in range(1, DSPAN + 1):

        @pl.when(me >= k)
        def _():
            part_copy(k).start()

        @pl.when(me + k > last)
        def _():
            parts_in[k - 1] = jnp.zeros((frames, LANES), F32)

    for k in range(1, DSPAN + 1):

        @pl.when(me + k <= last)
        def _():
            part_copy(k).wait_recv()

    series = part[span:, :]
    for k in range(DSPAN):
        series = series + parts_in[k]

    def pack(mean, second, peak):
        wide = lax.broadcasted_iota(jnp.int32, (1, LANES), 1)
        head = jnp.where(wide < trials, mean, pltpu.roll(second, trials, 1))
        return jnp.concatenate([head, peak], axis=0)

    def merge(slots, steps, count):
        heads = jnp.concatenate([slots[s, 0:1] for s in range(steps)], axis=0)
        peaks = jnp.concatenate([slots[s, 1:2] for s in range(steps)], axis=0)
        mean = jnp.sum(heads, axis=0, keepdims=True) / steps
        away = heads - mean
        second = pltpu.roll(mean * steps, trials, 1) + count * jnp.sum(away * away, axis=0, keepdims=True)
        return mean, second, jnp.max(peaks, axis=0, keepdims=True)

    mean = jnp.sum(series, axis=0, keepdims=True) / frames
    away = series - mean
    second_sum = jnp.sum(away * away, axis=0, keepdims=True)
    st_a[0] = pack(mean, second_sum, jnp.max(series, axis=0, keepdims=True))

    pair = send(st_a.at[0], st_a.at[1], pair_send, pair_recv, me + 1)

    @pl.when(core == 0)
    def _():
        pair.start()

    @pl.when(core == 1)
    def _():
        pair.wait_recv()
        st_b[0] = pack(*merge(st_a, CORES, float(frames)))
        pl.semaphore_wait(barrier, side - 1 + rings - 1)
        copies = [
            send(st_b.at[0], st_b.at[s], b_send.at[s - 1], b_recv.at[s - 1], col_peer(s))
            for s in range(1, side)
        ]
        for copy in copies:
            copy.start()
        for copy in copies:
            copy.wait_recv()
        st_c[0] = pack(*merge(st_b, side, float(frames * CORES)))
        spread_out = [
            send(st_c.at[0], st_c.at[s], c_send.at[2 * s + w], c_recv.at[s], row_peer(s, w))
            for s in range(1, rings)
            for w in (1, 0)
        ]
        spread_out.append(send(st_c.at[0], st_c.at[0], c_send.at[0], c_recv.at[0], me - 1))
        for copy in spread_out:
            copy.start()
        for s in range(1, rings):
            spread_out[2 * (s - 1)].wait_recv()

    @pl.when(core == 0)
    def _():
        for s in range(rings):
            send(st_c.at[0], st_c.at[s], c_send.at[s], c_recv.at[s], me + 1).wait_recv()

    average, second_sum, peak = merge(st_c, rings, float(frames * GROUP))
    variance = second_sum / (frames * tm_size)
    deviation = jnp.sqrt(variance + 1e-05)
    series = part[span:, :]
    for k in range(DSPAN):
        series = series + parts_in[k]
    z = (series - average) / deviation
    zout[...] = z[:, :trials]
    live = jnp.maximum(jnp.sum(mk[...].astype(F32)), 1.0)
    rows = jnp.concatenate([average / live, deviation / live, (peak - average) / deviation], axis=0)
    stats_out[...] = rows[:, :trials]

    @pl.when(me < last)
    def _():
        for k in range(4):
            halo(k).wait_send()

    for k in range(1, DSPAN + 1):

        @pl.when(me >= k)
        def _():
            part_copy(k).wait_send()

    @pl.when(core == 0)
    def _():
        pair.wait_send()

    @pl.when(core == 1)
    def _():
        for s in range(1, side):
            send(st_b.at[0], st_b.at[s], b_send.at[s - 1], b_recv.at[s - 1], col_peer(s)).wait_send()
        for s in range(1, rings):
            for w in (1, 0):
                send(st_c.at[0], st_c.at[s], c_send.at[2 * s + w], c_recv.at[s], row_peer(s, w)).wait_send()
        send(st_c.at[0], st_c.at[0], c_send.at[0], c_recv.at[0], me - 1).wait_send()


def per_device(tm_size, voltage, delays, chan_mask):
    frames = voltage.shape[2] // NCHAN
    trials = delays.shape[0]
    rows = voltage.shape[2] // HIGH
    volt = voltage.reshape(2, 2, rows, HIGH).transpose(0, 2, 1, 3).reshape(2, frames, 2 * LOW, HIGH)
    hist = TAPS - 1
    rings = tm_size // GROUP
    side = 2 * LOW * BLOCK
    vmem = pltpu.VMEM
    dma = pltpu.SemaphoreType.DMA
    span = DSPAN * frames
    zscore, stats = pl.pallas_call(
        functools.partial(kernel, tm_size, frames, trials),
        out_shape=(
            jax.ShapeDtypeStruct((frames, trials), F32),
            jax.ShapeDtypeStruct((3, trials), F32),
        ),
        in_specs=[pl.BlockSpec(memory_space=pl.ANY)] * 7,
        out_specs=(pl.BlockSpec(memory_space=pltpu.VMEM),) * 2,
        scratch_shapes=[
            vmem((2, hist + frames, 2 * LOW, HIGH), BF16),
            vmem((TAPS, 2 * LOW, HIGH), F32),
            vmem((2, side, side), BF16),
            vmem((2, LOW * BLOCK, HIGH), F32),
            vmem((2, 2 * HIGH, 2 * HIGH), BF16),
            vmem((trials, NCHAN), jnp.int32),
            vmem((1, NCHAN), jnp.int32),
            vmem((frames // BLOCK, side, 2 * LANES), BF16),
            vmem((frames // BLOCK, side, 2 * LANES), BF16),
            vmem((frames, NCHAN), BF16),
            vmem((NCHAN, LANES), F32),
            vmem((NCHAN, 2 * LANES), BF16),
            vmem((2, span + frames + 8, 2 * LANES), F32),
            vmem((span + frames, LANES), F32),
            vmem((DSPAN, frames, LANES), F32),
            vmem((CORES, 2, LANES), F32),
            vmem((GROUP // CORES, 2, LANES), F32),
            vmem((rings, 2, LANES), F32),
            dma((8,)),
            pltpu.SemaphoreType.REGULAR,
            pltpu.SemaphoreType.REGULAR,
            dma((4,)),
            dma((4,)),
            dma((DSPAN,)),
            dma((DSPAN,)),
            dma,
            dma,
            dma((GROUP // CORES - 1,)),
            dma((GROUP // CORES - 1,)),
            dma((2 * rings,)),
            dma((rings,)),
        ],
        compiler_params=pltpu.CompilerParams(
            collective_id=0, has_side_effects=True, vmem_limit_bytes=67043328
        ),
    )(
        volt, delays, chan_mask.reshape(1, NCHAN),
        jnp.asarray(filter_table()), jnp.asarray(first_table()),
        jnp.asarray(twist_table()), jnp.asarray(second_table()),
    )
    return zscore.T, stats


def solution(mesh):
    return jax.shard_map(
        functools.partial(per_device, mesh.shape["tm"]),
        mesh=mesh,
        in_specs=(P(None, None, ("beam", "tm")), P(), P("beam")),
        out_specs=(P(None, ("beam", "tm")), P(None, "beam")),
        check_vma=False,
    )
```

```python
import functools

import jax
import jax.numpy as jnp
import numpy as np
from jax import lax
from jax.experimental import pallas as pl
from jax.experimental.pallas import tpu as pltpu
from jax.sharding import PartitionSpec as P

NCHAN = 2048
TAPS = 16
LOW = 16
HIGH = 128
BLOCK = 8
GROUP = 16
LANES = 128
DSPAN = 3
CORES = 2
AHEAD = 4
MESH = pl.DeviceIdType.MESH
F32 = jnp.float32
BF16 = jnp.bfloat16
I16 = jnp.int16


def filter_table():
    length = TAPS * NCHAN
    position = np.arange(length, dtype=np.float64)
    centred = (position - (length - 1) / 2.0) / NCHAN
    window = 0.54 - 0.46 * np.cos(2.0 * np.pi * position / (length - 1))
    shaped = np.sinc(centred) * window
    shaped = shaped * np.sqrt(NCHAN / np.sum(shaped * shaped))
    rows = shaped.reshape(TAPS, LOW, 1, HIGH)
    return np.broadcast_to(rows, (TAPS, LOW, 2, HIGH)).reshape(TAPS, 2 * LOW, HIGH).astype(np.float32)


def split_table(table):
    high = table.astype(np.float32).astype(jnp.bfloat16)
    low = (table - high.astype(np.float64)).astype(np.float32).astype(jnp.bfloat16)
    return np.stack([high, low])


def first_table():
    angle = 2.0 * np.pi * (np.outer(np.arange(LOW), np.arange(LOW)) % LOW) / LOW
    turn = np.empty((2, LOW, LOW, 2))
    turn[0, :, :, 0] = np.cos(angle)
    turn[0, :, :, 1] = np.sin(angle)
    turn[1, :, :, 0] = -np.sin(angle)
    turn[1, :, :, 1] = np.cos(angle)
    full = np.zeros((2, LOW, BLOCK, BLOCK, LOW, 2))
    for frame in range(BLOCK):
        full[:, :, frame, frame] = turn
    side = 2 * LOW * BLOCK
    return split_table(full.reshape(side, side))


def twist_table():
    angle = 2.0 * np.pi * np.outer(np.arange(LOW), np.arange(HIGH)) / NCHAN
    both = np.stack([np.cos(angle), np.sin(angle)])
    return np.repeat(both, BLOCK, axis=1).astype(np.float32)


def second_table():
    angle = 2.0 * np.pi * (np.outer(np.arange(HIGH), np.arange(HIGH)) % HIGH) / HIGH
    top = np.concatenate([np.cos(angle), -np.sin(angle)], axis=1)
    bottom = np.concatenate([np.sin(angle), np.cos(angle)], axis=1)
    return split_table(np.concatenate([top, bottom], axis=0) / np.sqrt(NCHAN))


def dot(a, b):
    return jnp.dot(a, b, preferred_element_type=F32)


def kernel(
    tm_size, frames, trials,
    volt, delays, mask, coef, first, twist, second,
    zout, stats_out,
    x, c, b1, tw, b2, dl, mk, wh, wl, det, dt32, dtm, acc, part, parts_in, st_a, st_b,
    load_sem, near_sem, past_sem, halo_send, halo_recv, part_send, part_recv, pair_send, pair_recv,
    b_send, b_recv,
):
    me = lax.axis_index("tm")
    hist = TAPS - 1
    last = tm_size - 1
    rings = tm_size // GROUP
    side = GROUP // CORES
    core = lax.rem(me, CORES)
    place = me // CORES
    chips = rings * side

    def signal(sem, target):
        pl.semaphore_signal(sem, inc=1, device_id={"tm": target}, device_id_type=MESH)

    def send(source, target, send_sem, recv_sem, device):
        return pltpu.make_async_remote_copy(
            src_ref=source, dst_ref=target, send_sem=send_sem, recv_sem=recv_sem,
            device_id={"tm": device}, device_id_type=MESH,
        )

    def every_chip(act):
        def step(k, carry):
            chip = lax.rem(k, rings) * side + k // rings

            @pl.when(chip != place)
            def _():
                act(chip)

            return carry

        lax.fori_loop(0, chips, step, 0)

    barrier = pltpu.get_barrier_semaphore()

    @pl.when(core == 1)
    def _():
        signal(barrier, me - 1)

        @pl.when(me < last)
        def _():
            signal(barrier, me + 1)

    loads = [
        pltpu.make_async_copy(volt.at[p], x.at[p, pl.ds(hist, frames)], load_sem.at[p]) for p in range(2)
    ]
    for k, (source, target) in enumerate(
        [(coef, c), (first, b1), (twist, tw), (second, b2), (delays, dl), (mask, mk)]
    ):
        loads.append(pltpu.make_async_copy(source, target, load_sem.at[2 + k]))
    for load in loads:
        load.start()

    @pl.when(core == 0)
    def _():
        pl.semaphore_wait(barrier, 1 + jnp.minimum(me, 1))
        signal(near_sem, me + 1)

        @pl.when(me > 0)
        def _():
            signal(near_sem, me - 1)

    def halo(k):
        p, rows = k // 2, pl.ds((k % 2) * 16, 16)
        return send(
            x.at[p, pl.ds(frames, hist), rows], x.at[p, pl.ds(0, hist), rows],
            halo_send.at[k], halo_recv.at[k], me + 1,
        )

    loads[0].wait()
    loads[1].wait()

    @pl.when(core == 1)
    def _():
        pl.semaphore_wait(near_sem, 1 + jnp.minimum(last - me, 1))

    @pl.when(me < last)
    def _():
        for k in range(4):
            halo(k).start()

    @pl.when(me == 0)
    def _():
        x[:, :hist] = jnp.zeros((2, hist, 2 * LOW, HIGH), BF16)

    @pl.when(core == 1)
    def _():
        every_chip(lambda chip: signal(barrier, chip * CORES + 1))

    for load in loads[2:]:
        load.wait()

    def weigh(block, k):
        p, r = k // 2, lax.rem(k, 2)
        rows = pl.ds(pl.multiple_of(r * 16, 16), 16)
        lanes = pl.ds(pl.multiple_of(p * LANES, LANES), LANES)
        sums = [None] * BLOCK
        for i in range(BLOCK + hist):
            value = x[p, block * BLOCK + i, rows, :].astype(F32)
            for f in range(BLOCK):
                tap = i - f
                if 0 <= tap < TAPS:
                    term = c[tap, rows, :] * value
                    sums[f] = term if tap == 0 else sums[f] + term
                    if tap == TAPS - 1:
                        high = sums[f].astype(BF16)
                        low = (sums[f] - high.astype(F32)).astype(BF16)
                        spot = pl.ds(pl.multiple_of(f * 32 + r * 16, 16), 16)
                        wh[block, spot, lanes] = high
                        wl[block, spot, lanes] = low

    def transform(pair):
        half = LOW * BLOCK
        energies = []
        turns = [
            dot(b1[0], wh[b]) + dot(b1[0], wl[b]) + dot(b1[1], wh[b]) for b in (2 * pair, 2 * pair + 1)
        ]
        for z in turns:
            energy = None
            for p in range(2):
                zr = z[:half, p * LANES : (p + 1) * LANES]
                zi = z[half:, p * LANES : (p + 1) * LANES]
                turned = jnp.concatenate([zr * tw[0] + zi * tw[1], zi * tw[0] - zr * tw[1]], axis=1)
                high = turned.astype(BF16)
                low = (turned - high.astype(F32)).astype(BF16)
                u = dot(high, b2[0]) + dot(high, b2[1]) + dot(low, b2[0])
                power = u[:, :HIGH] * u[:, :HIGH] + u[:, HIGH:] * u[:, HIGH:]
                energy = power if p == 0 else energy + power
            energies.append(energy)
        for k in range(LOW):
            both = jnp.concatenate([e[k * BLOCK : (k + 1) * BLOCK] for e in energies], axis=0)
            det[2 * pair * BLOCK : 2 * (pair + 1) * BLOCK, k * HIGH : (k + 1) * HIGH] = both.astype(BF16)

    def late_half(k, carry):
        weigh(2, k)
        weigh(3, k)
        return carry

    lax.fori_loop(0, 4, late_half, 0)
    transform(1)

    used = jnp.where(mk[...] > 0, dl[...], -1).astype(F32).astype(BF16)
    lane = lax.broadcasted_iota(jnp.int32, (trials, LANES), 1)
    trial = lax.broadcasted_iota(jnp.int32, (trials, LANES), 0)
    spread = (lax.rem(lane, trials) == trial).astype(F32).astype(BF16)
    live = jnp.maximum(jnp.sum(mk[...].astype(F32)), 1.0)
    dt32[...] = lax.dot_general(used, spread, (((0,), (0,)), ((), ())), preferred_element_type=F32)
    lane_k = lax.broadcasted_iota(jnp.int32, (HIGH, LANES), 1)
    offset = (lane_k // trials).astype(F32)
    for k in range(LOW):
        rows = dt32[pl.ds(k, HIGH, stride=LOW), :] - offset
        dtm[k * HIGH : (k + 1) * HIGH, :LANES] = rows.astype(jnp.int32).astype(I16)
        dtm[k * HIGH : (k + 1) * HIGH, LANES:] = (rows - 2.0).astype(jnp.int32).astype(I16)
    acc[...] = jnp.zeros_like(acc)

    for k in range(4):

        @pl.when(me > 0)
        def _():
            halo(k).wait_recv()

        def early_half(block, carry):
            weigh(block, k)
            return carry

        lax.fori_loop(0, 2, early_half, 0)

    @pl.when(core == 0)
    def _():
        signal(past_sem, me + 1)

    transform(0)

    span = DSPAN * frames
    chunk = 2 * HIGH

    ones = jnp.ones((chunk, 2 * LANES), BF16)
    zeros = jnp.zeros((chunk, 2 * LANES), BF16)

    def select(base, h):
        target = jnp.full((chunk, 2 * LANES), base + 4 * h, jnp.int32).astype(I16)
        total = None
        for k in range(NCHAN // chunk):
            chosen = jnp.where(dtm[k * chunk : (k + 1) * chunk, :] == target, ones, zeros)
            term = dot(det[:, k * chunk : (k + 1) * chunk], chosen)
            total = term if k == 0 else total + term
        return total

    def shift(i, carry):
        totals = []
        for j in range(AHEAD):
            a = i * AHEAD + j
            totals.append([select(8 * a, h) for h in range(2)])
        for j in range(AHEAD):
            begin = pl.multiple_of(span - 8 * (i * AHEAD + j), 8)
            for h in range(2):
                acc[h, pl.ds(begin, frames), :] += totals[j][h]
        return carry

    lax.fori_loop(0, span // 8 // AHEAD, shift, 0)
    acc[0, 0:frames, :] += select(span, 0)

    even, odd = None, None
    rows_out = span + frames
    for h in range(2):
        for half in range(2):
            lanes = slice(half * LANES, (half + 1) * LANES)
            first_row = 4 * h + 2 * half
            left = acc[h, first_row : first_row + rows_out, lanes]
            right = acc[h, first_row + 1 : first_row + 1 + rows_out, lanes]
            even = left if even is None else even + left
            odd = right if odd is None else odd + right
    part[...] = even + pltpu.roll(odd, trials, 1)

    @pl.when(core == 1)
    def _():
        pl.semaphore_wait(past_sem, 1)

    def part_copy(k):
        return send(
            part.at[pl.ds(span - k * frames, frames)], parts_in.at[k - 1],
            part_send.at[k - 1], part_recv.at[k - 1], me - k,
        )

    for k in range(1, DSPAN + 1):

        @pl.when(me >= k)
        def _():
            part_copy(k).start()

        @pl.when(me + k > last)
        def _():
            parts_in[k - 1] = jnp.zeros((frames, LANES), F32)

    for k in range(1, DSPAN + 1):

        @pl.when(me + k <= last)
        def _():
            part_copy(k).wait_recv()

    series = part[span:, :]
    for k in range(DSPAN):
        series = series + parts_in[k]

    def pack(mean, second, peak):
        wide = lax.broadcasted_iota(jnp.int32, (1, LANES), 1)
        head = jnp.where(wide < trials, mean, pltpu.roll(second, trials, 1))
        return jnp.concatenate([head, peak], axis=0)

    def merge(slots, steps, count):
        entries = slots[...]
        mean = jnp.sum(entries, axis=0) / steps
        away = entries - mean[None]
        spread_sum = jnp.sum(away * away, axis=0)
        second = pltpu.roll(mean * steps, trials, 1) + count * spread_sum
        return mean[0:1], second[0:1], jnp.max(entries, axis=0)[1:2]

    mean = jnp.sum(series, axis=0, keepdims=True) / frames
    away = series - mean
    second_sum = jnp.sum(away * away, axis=0, keepdims=True)
    st_a[0] = pack(mean, second_sum, jnp.max(series, axis=0, keepdims=True))
    part[span:, :] = series

    @pl.when(core == 1)
    def _():
        pl.semaphore_wait(barrier, chips - 1)

    pair = send(st_a.at[0], st_a.at[1], pair_send, pair_recv, me + 1 - 2 * core)
    pair.start()
    pair.wait_recv()
    st_b[place] = pack(*merge(st_a, CORES, float(frames)))

    def chip_copy(chip):
        return send(st_b.at[place], st_b.at[place], b_send, b_recv, chip * CORES + core)

    every_chip(lambda chip: chip_copy(chip).start())
    others = st_b.at[pl.ds(0, chips - 1)]
    pltpu.make_async_copy(others, others, b_recv).wait()

    average, second_sum, peak = merge(st_b, chips, float(frames * CORES))
    variance = second_sum / (frames * tm_size)
    deviation = jnp.sqrt(variance + 1e-05)
    zout[...] = ((part[span:, :] - average) / deviation)[:, :trials]
    rows = jnp.concatenate([average / live, deviation / live, (peak - average) / deviation], axis=0)
    stats_out[...] = rows[:, :trials]

    pair.wait_send()
    pltpu.make_async_copy(others, others, b_send).wait()

    @pl.when(me < last)
    def _():
        for k in range(4):
            halo(k).wait_send()

    for k in range(1, DSPAN + 1):

        @pl.when(me >= k)
        def _():
            part_copy(k).wait_send()


def per_device(tm_size, voltage, delays, chan_mask):
    frames = voltage.shape[2] // NCHAN
    trials = delays.shape[0]
    rows = voltage.shape[2] // HIGH
    volt = voltage.reshape(2, 2, rows, HIGH).transpose(0, 2, 1, 3).reshape(2, frames, 2 * LOW, HIGH)
    hist = TAPS - 1
    side = 2 * LOW * BLOCK
    vmem = pltpu.VMEM
    dma = pltpu.SemaphoreType.DMA
    span = DSPAN * frames
    zscore, stats = pl.pallas_call(
        functools.partial(kernel, tm_size, frames, trials),
        out_shape=(
            jax.ShapeDtypeStruct((frames, trials), F32),
            jax.ShapeDtypeStruct((3, trials), F32),
        ),
        in_specs=[pl.BlockSpec(memory_space=pl.ANY)] * 7,
        out_specs=(pl.BlockSpec(memory_space=pltpu.VMEM),) * 2,
        scratch_shapes=[
            vmem((2, hist + frames, 2 * LOW, HIGH), BF16),
            vmem((TAPS, 2 * LOW, HIGH), F32),
            vmem((2, side, side), BF16),
            vmem((2, LOW * BLOCK, HIGH), F32),
            vmem((2, 2 * HIGH, 2 * HIGH), BF16),
            vmem((trials, NCHAN), jnp.int32),
            vmem((1, NCHAN), jnp.int32),
            vmem((frames // BLOCK, side, 2 * LANES), BF16),
            vmem((frames // BLOCK, side, 2 * LANES), BF16),
            vmem((frames, NCHAN), BF16),
            vmem((NCHAN, LANES), F32),
            vmem((NCHAN, 2 * LANES), I16),
            vmem((2, span + frames + 8, 2 * LANES), F32),
            vmem((span + frames, LANES), F32),
            vmem((DSPAN, frames, LANES), F32),
            vmem((CORES, 2, LANES), F32),
            vmem((tm_size // CORES, 2, LANES), F32),
            dma((8,)),
            pltpu.SemaphoreType.REGULAR,
            pltpu.SemaphoreType.REGULAR,
            dma((4,)),
            dma((4,)),
            dma((DSPAN,)),
            dma((DSPAN,)),
            dma,
            dma,
            dma,
            dma,
        ],
        compiler_params=pltpu.CompilerParams(
            collective_id=0, has_side_effects=True, vmem_limit_bytes=67043328
        ),
    )(
        volt, delays, chan_mask.reshape(1, NCHAN),
        jnp.asarray(filter_table()), jnp.asarray(first_table()),
        jnp.asarray(twist_table()), jnp.asarray(second_table()),
    )
    return zscore.T, stats


def solution(mesh):
    return jax.shard_map(
        functools.partial(per_device, mesh.shape["tm"]),
        mesh=mesh,
        in_specs=(P(None, None, ("beam", "tm")), P(), P("beam")),
        out_specs=(P(None, ("beam", "tm")), P(None, "beam")),
        check_vma=False,
    )
```

```python
import functools

import jax
import jax.numpy as jnp
import numpy as np
from jax import lax
from jax.experimental import pallas as pl
from jax.experimental.pallas import tpu as pltpu
from jax.sharding import PartitionSpec as P

NCHAN = 2048
TAPS = 16
LOW = 16
HIGH = 128
BLOCK = 8
GROUP = 16
LANES = 128
DSPAN = 3
CORES = 2
SOME = 9
MESH = pl.DeviceIdType.MESH
F32 = jnp.float32
BF16 = jnp.bfloat16
I16 = jnp.int16


def filter_table():
    length = TAPS * NCHAN
    position = np.arange(length, dtype=np.float64)
    centred = (position - (length - 1) / 2.0) / NCHAN
    window = 0.54 - 0.46 * np.cos(2.0 * np.pi * position / (length - 1))
    shaped = np.sinc(centred) * window
    shaped = shaped * np.sqrt(NCHAN / np.sum(shaped * shaped))
    rows = shaped.reshape(TAPS, LOW, 1, HIGH)
    return np.broadcast_to(rows, (TAPS, LOW, 2, HIGH)).reshape(TAPS, 2 * LOW, HIGH).astype(np.float32)


def split_table(table):
    high = table.astype(np.float32).astype(jnp.bfloat16)
    low = (table - high.astype(np.float64)).astype(np.float32).astype(jnp.bfloat16)
    return np.stack([high, low])


def first_table():
    angle = 2.0 * np.pi * (np.outer(np.arange(LOW), np.arange(LOW)) % LOW) / LOW
    turn = np.empty((2, LOW, LOW, 2))
    turn[0, :, :, 0] = np.cos(angle)
    turn[0, :, :, 1] = np.sin(angle)
    turn[1, :, :, 0] = -np.sin(angle)
    turn[1, :, :, 1] = np.cos(angle)
    full = np.zeros((2, LOW, BLOCK, BLOCK, LOW, 2))
    for frame in range(BLOCK):
        full[:, :, frame, frame] = turn
    side = 2 * LOW * BLOCK
    return split_table(full.reshape(side, side))


def twist_table():
    angle = 2.0 * np.pi * np.outer(np.arange(LOW), np.arange(HIGH)) / NCHAN
    both = np.stack([np.cos(angle), np.sin(angle)])
    return np.repeat(both, BLOCK, axis=1).astype(np.float32)


def second_table():
    angle = 2.0 * np.pi * (np.outer(np.arange(HIGH), np.arange(HIGH)) % HIGH) / HIGH
    top = np.concatenate([np.cos(angle), -np.sin(angle)], axis=1)
    bottom = np.concatenate([np.sin(angle), np.cos(angle)], axis=1)
    return split_table(np.concatenate([top, bottom], axis=0) / np.sqrt(NCHAN))


def dot(a, b):
    return jnp.dot(a, b, preferred_element_type=F32)


def kernel(
    tm_size, frames, trials,
    volt, delays, mask, coef, first, twist, second,
    zout, stats_out,
    x, c, b1, tw, b2, dl, mk, wh, wl, det, dt32, dtm, acc, part, parts_in, st_a, st_b,
    load_sem, go_sem, all_sem, past_sem, past2_sem, halo_send, halo_recv, part_send, part_recv, pair_send, pair_recv,
    b_send, b_recv,
):
    me = lax.axis_index("tm")
    hist = TAPS - 1
    last = tm_size - 1
    rings = tm_size // GROUP
    side = GROUP // CORES
    core = lax.rem(me, CORES)
    place = me // CORES
    chips = rings * side

    def signal(sem, target):
        pl.semaphore_signal(sem, inc=1, device_id={"tm": target}, device_id_type=MESH)

    def send(source, target, send_sem, recv_sem, device):
        return pltpu.make_async_remote_copy(
            src_ref=source, dst_ref=target, send_sem=send_sem, recv_sem=recv_sem,
            device_id={"tm": device}, device_id_type=MESH,
        )

    def every_chip(act):
        def step(k, carry):
            for j in range(1, SOME + 1):
                act(lax.rem(place + k * SOME + j, chips))
            return carry

        lax.fori_loop(0, (chips - 1) // SOME, step, 0)
        for j in range((chips - 1) // SOME * SOME + 1, chips):
            act(lax.rem(place + j, chips))

    barrier = pltpu.get_barrier_semaphore()

    @pl.when(me > 0)
    def _():
        signal(barrier, me - 1)

    @pl.when(me > 1)
    def _():
        signal(barrier, 0)

    early = frames - hist
    loads = [
        pltpu.make_async_copy(
            volt.at[p, pl.ds(begin, size)], x.at[p, pl.ds(hist + begin, size)], load_sem.at[2 * k + p]
        )
        for k, (begin, size) in enumerate([(early, hist), (0, early)])
        for p in range(2)
    ]
    for k, (source, target) in enumerate(
        [(coef, c), (first, b1), (twist, tw), (second, b2), (delays, dl), (mask, mk)]
    ):
        loads.append(pltpu.make_async_copy(source, target, load_sem.at[4 + k]))
    for load in loads:
        load.start()

    def halo(k):
        p, rows = k // 2, pl.ds((k % 2) * 16, 16)
        return send(
            x.at[p, pl.ds(frames, hist), rows], x.at[p, pl.ds(0, hist), rows],
            halo_send.at[k], halo_recv.at[k], me + 1,
        )

    loads[0].wait()
    loads[1].wait()

    @pl.when(me == 0)
    def _():
        pl.semaphore_wait(barrier, last)
        signal(go_sem, 1)

    @pl.when((me > 0) & (me < last))
    def _():
        pl.semaphore_wait(barrier, 1)

    @pl.when(me < last)
    def _():
        for k in range(4):
            halo(k).start()

    @pl.when(me == 0)
    def _():
        x[:, :hist] = jnp.zeros((2, hist, 2 * LOW, HIGH), BF16)

    for load in loads[2:]:
        load.wait()

    def weigh(block, k):
        p, r = k // 2, lax.rem(k, 2)
        rows = pl.ds(pl.multiple_of(r * 16, 16), 16)
        lanes = pl.ds(pl.multiple_of(p * LANES, LANES), LANES)
        sums = [None] * BLOCK
        for i in range(BLOCK + hist):
            value = x[p, block * BLOCK + i, rows, :].astype(F32)
            for f in range(BLOCK):
                tap = i - f
                if 0 <= tap < TAPS:
                    term = c[tap, rows, :] * value
                    sums[f] = term if tap == 0 else sums[f] + term
                    if tap == TAPS - 1:
                        high = sums[f].astype(BF16)
                        low = (sums[f] - high.astype(F32)).astype(BF16)
                        spot = pl.ds(pl.multiple_of(f * 32 + r * 16, 16), 16)
                        wh[block, spot, lanes] = high
                        wl[block, spot, lanes] = low

    def transform(pair):
        half = LOW * BLOCK
        energies = []
        turns = [
            dot(b1[0], wh[b]) + dot(b1[0], wl[b]) + dot(b1[1], wh[b]) for b in (2 * pair, 2 * pair + 1)
        ]
        for z in turns:
            energy = None
            for p in range(2):
                zr = z[:half, p * LANES : (p + 1) * LANES]
                zi = z[half:, p * LANES : (p + 1) * LANES]
                turned = jnp.concatenate([zr * tw[0] + zi * tw[1], zi * tw[0] - zr * tw[1]], axis=1)
                high = turned.astype(BF16)
                low = (turned - high.astype(F32)).astype(BF16)
                u = dot(high, b2[0]) + dot(high, b2[1]) + dot(low, b2[0])
                power = u[:, :HIGH] * u[:, :HIGH] + u[:, HIGH:] * u[:, HIGH:]
                energy = power if p == 0 else energy + power
            energies.append(energy)
        for k in range(LOW):
            both = jnp.concatenate([e[k * BLOCK : (k + 1) * BLOCK] for e in energies], axis=0)
            det[2 * pair * BLOCK : 2 * (pair + 1) * BLOCK, k * HIGH : (k + 1) * HIGH] = both.astype(BF16)

    def late_half(k, carry):
        weigh(2, k)
        weigh(3, k)
        return carry

    lax.fori_loop(0, 4, late_half, 0)
    transform(1)

    used = jnp.where(mk[...] > 0, dl[...], -1).astype(F32).astype(BF16)
    lane = lax.broadcasted_iota(jnp.int32, (trials, LANES), 1)
    trial = lax.broadcasted_iota(jnp.int32, (trials, LANES), 0)
    spread = (lax.rem(lane, trials) == trial).astype(F32).astype(BF16)
    live = jnp.maximum(jnp.sum(mk[...].astype(F32)), 1.0)
    dt32[...] = lax.dot_general(used, spread, (((0,), (0,)), ((), ())), preferred_element_type=F32)
    lane_k = lax.broadcasted_iota(jnp.int32, (HIGH, LANES), 1)
    offset = (lane_k // trials).astype(F32)
    for k in range(LOW):
        rows = dt32[pl.ds(k, HIGH, stride=LOW), :] - offset
        dtm[k * HIGH : (k + 1) * HIGH, :LANES] = rows.astype(jnp.int32).astype(I16)
        dtm[k * HIGH : (k + 1) * HIGH, LANES:] = (rows - 2.0).astype(jnp.int32).astype(I16)
    acc[...] = jnp.zeros_like(acc)

    @pl.when(me == 1)
    def _():
        pl.semaphore_wait(go_sem, 1)
        signal(past_sem, 2)
        signal(go_sem, DSPAN)

    for k in range(4):

        @pl.when(me > 0)
        def _():
            halo(k).wait_recv()

        def early_half(block, carry):
            weigh(block, k)
            return carry

        lax.fori_loop(0, 2, early_half, 0)

    @pl.when((me > 1) & (me < last))
    def _():
        signal(past_sem, me + 1)

    transform(0)

    def hear(parity):
        @pl.when((me > 1) & (core == parity))
        def _():
            pl.semaphore_wait(past_sem, 1)

            @pl.when(me < last)
            def _():
                signal(past2_sem, me + 1)

    hear(0)

    span = DSPAN * frames
    chunk = 2 * HIGH
    ahead = frames // 8

    ones = jnp.ones((chunk, 2 * LANES), BF16)
    zeros = jnp.zeros((chunk, 2 * LANES), BF16)

    def select(base, h):
        target = jnp.full((chunk, 2 * LANES), base + 4 * h, jnp.int32).astype(I16)
        total = None
        for k in range(NCHAN // chunk):
            chosen = jnp.where(dtm[k * chunk : (k + 1) * chunk, :] == target, ones, zeros)
            term = dot(det[:, k * chunk : (k + 1) * chunk], chosen)
            total = term if k == 0 else total + term
        return total

    def shift(i, carry):
        totals = []
        for j in range(ahead):
            a = i * ahead + j
            totals.append([select(8 * a, h) for h in range(2)])
        for j in range(ahead):
            begin = pl.multiple_of(span - 8 * (i * ahead + j), 8)
            for h in range(2):
                acc[h, pl.ds(begin, frames), :] += totals[j][h]
        return carry

    lax.fori_loop(0, jnp.minimum(me + 1, DSPAN), shift, 0)

    @pl.when(me >= DSPAN)
    def _():
        acc[0, 0:frames, :] += select(span, 0)


    hear(1)

    even, odd = None, None
    rows_out = span + frames
    for h in range(2):
        for half in range(2):
            lanes = slice(half * LANES, (half + 1) * LANES)
            first_row = 4 * h + 2 * half
            left = acc[h, first_row : first_row + rows_out, lanes]
            right = acc[h, first_row + 1 : first_row + 1 + rows_out, lanes]
            even = left if even is None else even + left
            odd = right if odd is None else odd + right
    part[...] = even + pltpu.roll(odd, trials, 1)

    def part_copy(k):
        return send(
            part.at[pl.ds(span - k * frames, frames)], parts_in.at[k - 1],
            part_send.at[k - 1], part_recv.at[k - 1], me - k,
        )

    for k in range(1, DSPAN + 1):

        @pl.when(me >= k)
        def _():
            if k == DSPAN:
                pl.semaphore_wait(past2_sem, 1)
            part_copy(k).start()

        @pl.when(me + k > last)
        def _():
            parts_in[k - 1] = jnp.zeros((frames, LANES), F32)

    @pl.when(me == DSPAN)
    def _():
        pl.semaphore_wait(go_sem, 1)

        def tell(k, carry):
            for j in range(SOME):
                signal(all_sem, DSPAN + 1 + k * SOME + j)
            return carry

        others = tm_size - 1 - DSPAN
        signal(all_sem, 2)
        lax.fori_loop(0, others // SOME, tell, 0)
        for j in range(others // SOME * SOME, others):
            signal(all_sem, DSPAN + 1 + j)

    for k in range(1, DSPAN + 1):

        @pl.when(me + k <= last)
        def _():
            part_copy(k).wait_recv()

    series = part[span:, :]
    for k in range(DSPAN):
        series = series + parts_in[k]

    def pack(mean, second, peak):
        wide = lax.broadcasted_iota(jnp.int32, (1, LANES), 1)
        head = jnp.where(wide < trials, mean, pltpu.roll(second, trials, 1))
        return jnp.concatenate([head, peak], axis=0)

    def merge(slots, steps, count):
        entries = slots[...]
        mean = jnp.sum(entries, axis=0) / steps
        away = entries - mean[None]
        spread_sum = jnp.sum(away * away, axis=0)
        second = pltpu.roll(mean * steps, trials, 1) + count * spread_sum
        return mean[0:1], second[0:1], jnp.max(entries, axis=0)[1:2]

    mean = jnp.sum(series, axis=0, keepdims=True) / frames
    away = series - mean
    second_sum = jnp.sum(away * away, axis=0, keepdims=True)
    st_a[0] = pack(mean, second_sum, jnp.max(series, axis=0, keepdims=True))
    part[span:, :] = series

    @pl.when((me > 1) & (me != DSPAN))
    def _():
        pl.semaphore_wait(all_sem, 1)

    pair = send(st_a.at[0], st_a.at[1], pair_send, pair_recv, me + 1 - 2 * core)
    pair.start()
    pair.wait_recv()
    st_b[place] = pack(*merge(st_a, CORES, float(frames)))

    def chip_copy(chip):
        return send(st_b.at[place], st_b.at[place], b_send, b_recv, chip * CORES + core)

    every_chip(lambda chip: chip_copy(chip).start())
    others = st_b.at[pl.ds(0, chips - 1)]
    pltpu.make_async_copy(others, others, b_recv).wait()

    average, second_sum, peak = merge(st_b, chips, float(frames * CORES))
    variance = second_sum / (frames * tm_size)
    deviation = jnp.sqrt(variance + 1e-05)
    zout[...] = ((part[span:, :] - average) / deviation)[:, :trials]
    rows = jnp.concatenate([average / live, deviation / live, (peak - average) / deviation], axis=0)
    stats_out[...] = rows[:, :trials]

    pair.wait_send()
    pltpu.make_async_copy(others, others, b_send).wait()

    @pl.when(me < last)
    def _():
        for k in range(4):
            halo(k).wait_send()

    for k in range(1, DSPAN + 1):

        @pl.when(me >= k)
        def _():
            part_copy(k).wait_send()


def per_device(tm_size, voltage, delays, chan_mask):
    frames = voltage.shape[2] // NCHAN
    trials = delays.shape[0]
    rows = voltage.shape[2] // HIGH
    volt = voltage.reshape(2, 2, rows, HIGH).transpose(0, 2, 1, 3).reshape(2, frames, 2 * LOW, HIGH)
    hist = TAPS - 1
    side = 2 * LOW * BLOCK
    vmem = pltpu.VMEM
    dma = pltpu.SemaphoreType.DMA
    span = DSPAN * frames
    zscore, stats = pl.pallas_call(
        functools.partial(kernel, tm_size, frames, trials),
        out_shape=(
            jax.ShapeDtypeStruct((frames, trials), F32),
            jax.ShapeDtypeStruct((3, trials), F32),
        ),
        in_specs=[pl.BlockSpec(memory_space=pl.ANY)] * 7,
        out_specs=(pl.BlockSpec(memory_space=pltpu.VMEM),) * 2,
        scratch_shapes=[
            vmem((2, hist + frames, 2 * LOW, HIGH), BF16),
            vmem((TAPS, 2 * LOW, HIGH), F32),
            vmem((2, side, side), BF16),
            vmem((2, LOW * BLOCK, HIGH), F32),
            vmem((2, 2 * HIGH, 2 * HIGH), BF16),
            vmem((trials, NCHAN), jnp.int32),
            vmem((1, NCHAN), jnp.int32),
            vmem((frames // BLOCK, side, 2 * LANES), BF16),
            vmem((frames // BLOCK, side, 2 * LANES), BF16),
            vmem((frames, NCHAN), BF16),
            vmem((NCHAN, LANES), F32),
            vmem((NCHAN, 2 * LANES), I16),
            vmem((2, span + frames + 8, 2 * LANES), F32),
            vmem((span + frames, LANES), F32),
            vmem((DSPAN, frames, LANES), F32),
            vmem((CORES, 2, LANES), F32),
            vmem((tm_size // CORES, 2, LANES), F32),
            dma((10,)),
            pltpu.SemaphoreType.REGULAR,
            pltpu.SemaphoreType.REGULAR,
            pltpu.SemaphoreType.REGULAR,
            pltpu.SemaphoreType.REGULAR,
            dma((4,)),
            dma((4,)),
            dma((DSPAN,)),
            dma((DSPAN,)),
            dma,
            dma,
            dma,
            dma,
        ],
        compiler_params=pltpu.CompilerParams(
            collective_id=0, has_side_effects=True, vmem_limit_bytes=40 << 20
        ),
    )(
        *(
            pltpu.with_memory_space_constraint(value, pltpu.HBM)
            for value in (
                volt, delays, chan_mask.reshape(1, NCHAN),
                jnp.asarray(filter_table()), jnp.asarray(first_table()),
                jnp.asarray(twist_table()), jnp.asarray(second_table()),
            )
        )
    )
    return zscore.T, stats


def solution(mesh):
    return jax.shard_map(
        functools.partial(per_device, mesh.shape["tm"]),
        mesh=mesh,
        in_specs=(P(None, None, ("beam", "tm")), P(), P("beam")),
        out_specs=(P(None, ("beam", "tm")), P(None, "beam")),
        check_vma=False,
    )
```

```python
import functools

import jax
import jax.numpy as jnp
import numpy as np
from jax import lax
from jax.experimental import pallas as pl
from jax.experimental.pallas import tpu as pltpu
from jax.sharding import PartitionSpec as P

NCHAN = 2048
TAPS = 16
LOW = 16
HIGH = 128
BLOCK = 8
GROUP = 16
LANES = 128
DSPAN = 3
CORES = 2
SOME = 9
MESH = pl.DeviceIdType.MESH
F32 = jnp.float32
BF16 = jnp.bfloat16
I16 = jnp.int16
F8 = jnp.float8_e4m3fn


def filter_table():
    length = TAPS * NCHAN
    position = np.arange(length, dtype=np.float64)
    centred = (position - (length - 1) / 2.0) / NCHAN
    window = 0.54 - 0.46 * np.cos(2.0 * np.pi * position / (length - 1))
    shaped = np.sinc(centred) * window
    shaped = shaped * np.sqrt(NCHAN / np.sum(shaped * shaped))
    rows = shaped.reshape(TAPS, LOW, 1, HIGH)
    return np.broadcast_to(rows, (TAPS, LOW, 2, HIGH)).reshape(TAPS, 2 * LOW, HIGH).astype(np.float32)


def split_table(table):
    high = table.astype(np.float32).astype(jnp.bfloat16)
    low = (table - high.astype(np.float64)).astype(np.float32).astype(jnp.bfloat16)
    return np.stack([high, low])


def first_table():
    angle = 2.0 * np.pi * (np.outer(np.arange(LOW), np.arange(LOW)) % LOW) / LOW
    turn = np.empty((2, LOW, LOW, 2))
    turn[0, :, :, 0] = np.cos(angle)
    turn[0, :, :, 1] = np.sin(angle)
    turn[1, :, :, 0] = -np.sin(angle)
    turn[1, :, :, 1] = np.cos(angle)
    full = np.zeros((2, LOW, BLOCK, BLOCK, LOW, 2))
    for frame in range(BLOCK):
        full[:, :, frame, frame] = turn
    side = 2 * LOW * BLOCK
    return split_table(full.reshape(side, side))


def twist_table():
    angle = 2.0 * np.pi * np.outer(np.arange(LOW), np.arange(HIGH)) / NCHAN
    both = np.stack([np.cos(angle), np.sin(angle)])
    return np.repeat(both, BLOCK, axis=1).astype(np.float32)


def second_table():
    angle = 2.0 * np.pi * (np.outer(np.arange(HIGH), np.arange(HIGH)) % HIGH) / HIGH
    top = np.concatenate([np.cos(angle), -np.sin(angle)], axis=1)
    bottom = np.concatenate([np.sin(angle), np.cos(angle)], axis=1)
    return split_table(np.concatenate([top, bottom], axis=0) / np.sqrt(NCHAN))


def dot(a, b):
    return lax.dot_general(a, b, (((1,), (0,)), ((), ())), preferred_element_type=F32)


def hand_on(zscore, stats, zout, stats_out, sems):
    copies = [pltpu.make_async_copy(zscore, zout, sems.at[0]), pltpu.make_async_copy(stats, stats_out, sems.at[1])]
    for copy in copies:
        copy.start()
    for copy in copies:
        copy.wait()


def kernel(
    tm_size, frames, trials,
    volt, delays, mask, coef, first, twist, second,
    zout, stats_out,
    x, c, b1, tw, b2, dl, mk, wh, wl, det, dt32, dtm, acc, part, parts_in, st_a, st_b,
    load_sem, go_sem, all_sem, past_sem, past2_sem, halo_send, halo_recv, part_send, part_recv, pair_send, pair_recv,
    b_send, b_recv,
):
    me = lax.axis_index("tm")
    hist = TAPS - 1
    last = tm_size - 1
    rings = tm_size // GROUP
    side = GROUP // CORES
    core = lax.rem(me, CORES)
    place = me // CORES
    chips = rings * side

    def signal(sem, target):
        pl.semaphore_signal(sem, inc=1, device_id={"tm": target}, device_id_type=MESH)

    def send(source, target, send_sem, recv_sem, device):
        return pltpu.make_async_remote_copy(
            src_ref=source, dst_ref=target, send_sem=send_sem, recv_sem=recv_sem,
            device_id={"tm": device}, device_id_type=MESH,
        )

    def every_chip(act):
        def step(k, carry):
            for j in range(1, SOME + 1):
                act(lax.rem(place + k * SOME + j, chips))
            return carry

        lax.fori_loop(0, (chips - 1) // SOME, step, 0)
        for j in range((chips - 1) // SOME * SOME + 1, chips):
            act(lax.rem(place + j, chips))

    barrier = pltpu.get_barrier_semaphore()

    @pl.when(me > 0)
    def _():
        signal(barrier, me - 1)

    @pl.when(me > 1)
    def _():
        signal(barrier, 0)

    early = frames - hist
    loads = [
        pltpu.make_async_copy(
            volt.at[p, pl.ds(begin, size)], x.at[p, pl.ds(hist + begin, size)], load_sem.at[2 * k + p]
        )
        for k, (begin, size) in enumerate([(early, hist), (0, early)])
        for p in range(2)
    ]
    for k, (source, target) in enumerate(
        [(coef, c), (first, b1), (twist, tw), (second, b2), (delays, dl), (mask, mk)]
    ):
        loads.append(pltpu.make_async_copy(source, target, load_sem.at[4 + k]))
    for load in loads:
        load.start()

    def halo(k):
        p, rows = k // 2, pl.ds((k % 2) * 16, 16)
        return send(
            x.at[p, pl.ds(frames, hist), rows], x.at[p, pl.ds(0, hist), rows],
            halo_send.at[k], halo_recv.at[k], me + 1,
        )

    loads[0].wait()
    loads[1].wait()

    @pl.when(me == 0)
    def _():
        pl.semaphore_wait(barrier, last)
        signal(go_sem, 1)

    @pl.when((me > 0) & (me < last))
    def _():
        pl.semaphore_wait(barrier, 1)

    @pl.when(me < last)
    def _():
        for k in range(4):
            halo(k).start()

    @pl.when(me == 0)
    def _():
        x[:, :hist] = jnp.zeros((2, hist, 2 * LOW, HIGH), BF16)

    for load in loads[2:]:
        load.wait()

    def weigh(block, k):
        p, r = k // 2, lax.rem(k, 2)
        rows = pl.ds(pl.multiple_of(r * 16, 16), 16)
        lanes = pl.ds(pl.multiple_of(p * LANES, LANES), LANES)
        sums = [None] * BLOCK
        for i in range(BLOCK + hist):
            value = x[p, block * BLOCK + i, rows, :].astype(F32)
            for f in range(BLOCK):
                tap = i - f
                if 0 <= tap < TAPS:
                    term = c[tap, rows, :] * value
                    sums[f] = term if tap == 0 else sums[f] + term
                    if tap == TAPS - 1:
                        high = sums[f].astype(BF16)
                        low = (sums[f] - high.astype(F32)).astype(BF16)
                        spot = pl.ds(pl.multiple_of(f * 32 + r * 16, 16), 16)
                        wh[block, spot, lanes] = high
                        wl[block, spot, lanes] = low

    def transform(pair):
        half = LOW * BLOCK
        energies = []
        turns = [
            dot(b1[0], wh[b]) + dot(b1[0], wl[b]) + dot(b1[1], wh[b]) for b in (2 * pair, 2 * pair + 1)
        ]
        for z in turns:
            energy = None
            for p in range(2):
                zr = z[:half, p * LANES : (p + 1) * LANES]
                zi = z[half:, p * LANES : (p + 1) * LANES]
                turned = jnp.concatenate([zr * tw[0] + zi * tw[1], zi * tw[0] - zr * tw[1]], axis=1)
                high = turned.astype(BF16)
                low = (turned - high.astype(F32)).astype(BF16)
                u = dot(high, b2[0]) + dot(high, b2[1]) + dot(low, b2[0])
                power = u[:, :HIGH] * u[:, :HIGH] + u[:, HIGH:] * u[:, HIGH:]
                energy = power if p == 0 else energy + power
            energies.append(energy)
        for k in range(LOW):
            both = jnp.concatenate([e[k * BLOCK : (k + 1) * BLOCK] for e in energies], axis=0)
            det[2 * pair * BLOCK : 2 * (pair + 1) * BLOCK, k * HIGH : (k + 1) * HIGH] = both.astype(BF16)

    def late_half(k, carry):
        weigh(2, k)
        weigh(3, k)
        return carry

    lax.fori_loop(0, 4, late_half, 0)
    transform(1)

    used = jnp.where(mk[...] > 0, dl[...], -1).astype(F32).astype(BF16)
    lane = lax.broadcasted_iota(jnp.int32, (trials, LANES), 1)
    trial = lax.broadcasted_iota(jnp.int32, (trials, LANES), 0)
    spread = (lax.rem(lane, trials) == trial).astype(F32).astype(BF16)
    live = jnp.maximum(jnp.sum(mk[...].astype(F32)), 1.0)
    dt32[...] = lax.dot_general(used, spread, (((0,), (0,)), ((), ())), preferred_element_type=F32)
    lane_k = lax.broadcasted_iota(jnp.int32, (HIGH, LANES), 1)
    offset = (lane_k // trials).astype(F32)
    for k in range(LOW):
        rows = dt32[pl.ds(k, HIGH, stride=LOW), :] - offset
        dtm[k * HIGH : (k + 1) * HIGH, :LANES] = rows.astype(jnp.int32).astype(I16)
        dtm[k * HIGH : (k + 1) * HIGH, LANES:] = (rows - 2.0).astype(jnp.int32).astype(I16)
    acc[...] = jnp.zeros_like(acc)

    span = DSPAN * frames
    chunk = 2 * HIGH
    ahead = frames // 8
    part_rows = frames // 2

    ones = jnp.ones((chunk, 2 * LANES), BF16)
    zeros = jnp.zeros((chunk, 2 * LANES), BF16)

    def select(begin, size, base, h):
        target = jnp.full((chunk, 2 * LANES), base + 4 * h, jnp.int32).astype(I16)
        total = None
        for k in range(NCHAN // chunk):
            chosen = jnp.where(dtm[k * chunk : (k + 1) * chunk, :] == target, ones, zeros).astype(F8)
            term = dot(det[begin : begin + size, k * chunk : (k + 1) * chunk], chosen)
            total = term if k == 0 else total + term
        return total

    def shifts(first_row, size):
        def shift(i, carry):
            totals = []
            for j in range(ahead):
                a = i * ahead + j
                totals.append([select(first_row, size, 8 * a, h) for h in range(2)])
            for j in range(ahead):
                begin = pl.multiple_of(span + first_row - 8 * (i * ahead + j), 8)
                for h in range(2):
                    acc[h, pl.ds(begin, size), :] += totals[j][h]
            return carry

        lax.fori_loop(0, jnp.minimum(me + 1, DSPAN), shift, 0)

        @pl.when(me >= DSPAN)
        def _():
            acc[0, first_row : first_row + size, :] += select(first_row, size, span, 0)

    fed_late = (me > 0) & (lax.rem(me, CORES * side) == 0)

    @pl.when(fed_late)
    def _():
        shifts(part_rows, part_rows)

    @pl.when(me == 1)
    def _():
        pl.semaphore_wait(go_sem, 1)
        signal(past_sem, 2)
        signal(go_sem, DSPAN)

    for k in range(4):

        @pl.when(me > 0)
        def _():
            halo(k).wait_recv()

        def early_half(block, carry):
            weigh(block, k)
            return carry

        lax.fori_loop(0, 2, early_half, 0)

    @pl.when((me > 1) & (me < last))
    def _():
        signal(past_sem, me + 1)

    transform(0)

    def hear(parity):
        @pl.when((me > 1) & (core == parity))
        def _():
            pl.semaphore_wait(past_sem, 1)

            @pl.when(me < last)
            def _():
                signal(past2_sem, me + 1)

    hear(0)

    @pl.when(fed_late)
    def _():
        shifts(0, part_rows)

    @pl.when(jnp.logical_not(fed_late))
    def _():
        shifts(0, frames)

    hear(1)

    even, odd = None, None
    rows_out = span + frames
    for h in range(2):
        for half in range(2):
            lanes = slice(half * LANES, (half + 1) * LANES)
            first_row = 4 * h + 2 * half
            left = acc[h, first_row : first_row + rows_out, lanes]
            right = acc[h, first_row + 1 : first_row + 1 + rows_out, lanes]
            even = left if even is None else even + left
            odd = right if odd is None else odd + right
    part[...] = even + pltpu.roll(odd, trials, 1)

    def part_copy(k):
        return send(
            part.at[pl.ds(span - k * frames, frames)], parts_in.at[k - 1],
            part_send.at[k - 1], part_recv.at[k - 1], me - k,
        )

    for k in range(1, DSPAN + 1):

        @pl.when(me >= k)
        def _():
            if k == DSPAN:
                pl.semaphore_wait(past2_sem, 1)
            part_copy(k).start()

        @pl.when(me + k > last)
        def _():
            parts_in[k - 1] = jnp.zeros((frames, LANES), F32)

    @pl.when(me == DSPAN)
    def _():
        pl.semaphore_wait(go_sem, 1)

        def tell(k, carry):
            for j in range(SOME):
                signal(all_sem, DSPAN + 1 + k * SOME + j)
            return carry

        others = tm_size - 1 - DSPAN
        signal(all_sem, 2)
        lax.fori_loop(0, others // SOME, tell, 0)
        for j in range(others // SOME * SOME, others):
            signal(all_sem, DSPAN + 1 + j)

    for k in range(1, DSPAN + 1):

        @pl.when(me + k <= last)
        def _():
            part_copy(k).wait_recv()

    series = part[span:, :]
    for k in range(DSPAN):
        series = series + parts_in[k]

    def pack(mean, second, peak):
        wide = lax.broadcasted_iota(jnp.int32, (1, LANES), 1)
        head = jnp.where(wide < trials, mean, pltpu.roll(second, trials, 1))
        return jnp.concatenate([head, peak], axis=0)

    def merge(slots, steps, count):
        entries = slots[...]
        mean = jnp.sum(entries, axis=0) / steps
        away = entries - mean[None]
        spread_sum = jnp.sum(away * away, axis=0)
        second = pltpu.roll(mean * steps, trials, 1) + count * spread_sum
        return mean[0:1], second[0:1], jnp.max(entries, axis=0)[1:2]

    mean = jnp.sum(series, axis=0, keepdims=True) / frames
    away = series - mean
    second_sum = jnp.sum(away * away, axis=0, keepdims=True)
    st_a[0] = pack(mean, second_sum, jnp.max(series, axis=0, keepdims=True))
    part[span:, :] = series

    @pl.when((me > 1) & (me != DSPAN))
    def _():
        pl.semaphore_wait(all_sem, 1)

    pair = send(st_a.at[0], st_a.at[1], pair_send, pair_recv, me + 1 - 2 * core)
    pair.start()
    pair.wait_recv()
    st_b[place] = pack(*merge(st_a, CORES, float(frames)))

    def chip_copy(chip):
        return send(st_b.at[place], st_b.at[place], b_send, b_recv, chip * CORES + core)

    every_chip(lambda chip: chip_copy(chip).start())
    others = st_b.at[pl.ds(0, chips - 1)]
    pltpu.make_async_copy(others, others, b_recv).wait()

    average, second_sum, peak = merge(st_b, chips, float(frames * CORES))
    variance = second_sum / (frames * tm_size)
    deviation = jnp.sqrt(variance + 1e-05)
    zout[...] = ((part[span:, :] - average) / deviation)[:, :trials]
    rows = jnp.concatenate([average / live, deviation / live, (peak - average) / deviation], axis=0)
    stats_out[...] = rows[:, :trials]

    pair.wait_send()
    pltpu.make_async_copy(others, others, b_send).wait()

    @pl.when(me < last)
    def _():
        for k in range(4):
            halo(k).wait_send()

    for k in range(1, DSPAN + 1):

        @pl.when(me >= k)
        def _():
            part_copy(k).wait_send()


def per_device(tm_size, voltage, delays, chan_mask):
    frames = voltage.shape[2] // NCHAN
    trials = delays.shape[0]
    rows = voltage.shape[2] // HIGH
    volt = voltage.reshape(2, 2, rows, HIGH).transpose(0, 2, 1, 3).reshape(2, frames, 2 * LOW, HIGH)
    hist = TAPS - 1
    side = 2 * LOW * BLOCK
    vmem = pltpu.VMEM
    dma = pltpu.SemaphoreType.DMA
    span = DSPAN * frames
    zscore, stats = pl.pallas_call(
        functools.partial(kernel, tm_size, frames, trials),
        out_shape=(
            jax.ShapeDtypeStruct((frames, trials), F32),
            jax.ShapeDtypeStruct((3, trials), F32),
        ),
        in_specs=[pl.BlockSpec(memory_space=pl.ANY)] * 7,
        out_specs=(pl.BlockSpec(memory_space=pltpu.VMEM),) * 2,
        scratch_shapes=[
            vmem((2, hist + frames, 2 * LOW, HIGH), BF16),
            vmem((TAPS, 2 * LOW, HIGH), F32),
            vmem((2, side, side), BF16),
            vmem((2, LOW * BLOCK, HIGH), F32),
            vmem((2, 2 * HIGH, 2 * HIGH), BF16),
            vmem((trials, NCHAN), jnp.int32),
            vmem((1, NCHAN), jnp.int32),
            vmem((frames // BLOCK, side, 2 * LANES), BF16),
            vmem((frames // BLOCK, side, 2 * LANES), BF16),
            vmem((frames, NCHAN), BF16),
            vmem((NCHAN, LANES), F32),
            vmem((NCHAN, 2 * LANES), I16),
            vmem((2, span + frames + 8, 2 * LANES), F32),
            vmem((span + frames, LANES), F32),
            vmem((DSPAN, frames, LANES), F32),
            vmem((CORES, 2, LANES), F32),
            vmem((tm_size // CORES, 2, LANES), F32),
            dma((10,)),
            pltpu.SemaphoreType.REGULAR,
            pltpu.SemaphoreType.REGULAR,
            pltpu.SemaphoreType.REGULAR,
            pltpu.SemaphoreType.REGULAR,
            dma((4,)),
            dma((4,)),
            dma((DSPAN,)),
            dma((DSPAN,)),
            dma,
            dma,
            dma,
            dma,
        ],
        compiler_params=pltpu.CompilerParams(
            collective_id=0, has_side_effects=True, vmem_limit_bytes=40 << 20
        ),
    )(
        *(
            pltpu.with_memory_space_constraint(value, pltpu.HBM)
            for value in (
                volt, delays, chan_mask.reshape(1, NCHAN),
                jnp.asarray(filter_table()), jnp.asarray(first_table()),
                jnp.asarray(twist_table()), jnp.asarray(second_table()),
            )
        )
    )
    zscore, stats = pl.pallas_call(
        hand_on,
        out_shape=(
            jax.ShapeDtypeStruct((frames, trials), F32),
            jax.ShapeDtypeStruct((3, trials), F32),
        ),
        in_specs=[pl.BlockSpec(memory_space=pltpu.VMEM)] * 2,
        out_specs=(pl.BlockSpec(memory_space=pl.ANY),) * 2,
        scratch_shapes=[dma((2,))],
        compiler_params=pltpu.CompilerParams(vmem_limit_bytes=1 << 20),
    )(zscore, stats)
    return zscore.T, stats


def solution(mesh):
    return jax.shard_map(
        functools.partial(per_device, mesh.shape["tm"]),
        mesh=mesh,
        in_specs=(P(None, None, ("beam", "tm")), P(), P("beam")),
        out_specs=(P(None, ("beam", "tm")), P(None, "beam")),
        check_vma=False,
    )
```

```python
import functools

import jax
import jax.numpy as jnp
import numpy as np
from jax import lax
from jax.experimental import pallas as pl
from jax.experimental.pallas import tpu as pltpu
from jax.sharding import PartitionSpec as P

NCHAN = 2048
TAPS = 16
LOW = 16
HIGH = 128
BLOCK = 8
GROUP = 16
LANES = 128
DSPAN = 3
CORES = 2
SOME = 9
MESH = pl.DeviceIdType.MESH
F32 = jnp.float32
BF16 = jnp.bfloat16
I16 = jnp.int16
F8 = jnp.float8_e4m3fn


def filter_table():
    length = TAPS * NCHAN
    position = np.arange(length, dtype=np.float64)
    centred = (position - (length - 1) / 2.0) / NCHAN
    window = 0.54 - 0.46 * np.cos(2.0 * np.pi * position / (length - 1))
    shaped = np.sinc(centred) * window
    shaped = shaped * np.sqrt(NCHAN / np.sum(shaped * shaped))
    rows = shaped.reshape(TAPS, LOW, 1, HIGH)
    return np.broadcast_to(rows, (TAPS, LOW, 2, HIGH)).reshape(TAPS, 2 * LOW, HIGH).astype(np.float32)


def split_table(table):
    high = table.astype(np.float32).astype(jnp.bfloat16)
    low = (table - high.astype(np.float64)).astype(np.float32).astype(jnp.bfloat16)
    return np.stack([high, low])


def first_table():
    angle = 2.0 * np.pi * (np.outer(np.arange(LOW), np.arange(LOW)) % LOW) / LOW
    turn = np.empty((2, LOW, LOW, 2))
    turn[0, :, :, 0] = np.cos(angle)
    turn[0, :, :, 1] = np.sin(angle)
    turn[1, :, :, 0] = -np.sin(angle)
    turn[1, :, :, 1] = np.cos(angle)
    full = np.zeros((2, LOW, BLOCK, BLOCK, LOW, 2))
    for frame in range(BLOCK):
        full[:, :, frame, frame] = turn
    side = 2 * LOW * BLOCK
    return split_table(full.reshape(side, side))


def twist_table():
    angle = 2.0 * np.pi * np.outer(np.arange(LOW), np.arange(HIGH)) / NCHAN
    both = np.stack([np.cos(angle), np.sin(angle)])
    return np.repeat(both, BLOCK, axis=1).astype(np.float32)


def second_table():
    angle = 2.0 * np.pi * (np.outer(np.arange(HIGH), np.arange(HIGH)) % HIGH) / HIGH
    top = np.concatenate([np.cos(angle), -np.sin(angle)], axis=1)
    bottom = np.concatenate([np.sin(angle), np.cos(angle)], axis=1)
    return split_table(np.concatenate([top, bottom], axis=0) / np.sqrt(NCHAN))


def dot(a, b):
    return lax.dot_general(a, b, (((1,), (0,)), ((), ())), preferred_element_type=F32)


def hand_on(zscore, stats, zout, stats_out, sems):
    copies = [pltpu.make_async_copy(zscore, zout, sems.at[0]), pltpu.make_async_copy(stats, stats_out, sems.at[1])]
    for copy in copies:
        copy.start()
    for copy in copies:
        copy.wait()


def kernel(
    tm_size, frames, trials,
    volt, delays, mask, coef, first, twist, second,
    zout, stats_out,
    x, c, b1, tw, b2, dl, mk, wh, wl, det, dt32, dtm, sel, acc, part, parts_in, st_a, st_b,
    load_sem, go_sem, all_sem, past_sem, past2_sem, halo_send, halo_recv, part_send, part_recv, pair_send, pair_recv,
    b_send, b_recv,
):
    me = lax.axis_index("tm")
    hist = TAPS - 1
    last = tm_size - 1
    rings = tm_size // GROUP
    side = GROUP // CORES
    core = lax.rem(me, CORES)
    place = me // CORES
    row, col = place // side, lax.rem(place, side)
    chips = rings * side

    def signal(sem, target):
        pl.semaphore_signal(sem, inc=1, device_id={"tm": target}, device_id_type=MESH)

    def send(source, target, send_sem, recv_sem, device):
        return pltpu.make_async_remote_copy(
            src_ref=source, dst_ref=target, send_sem=send_sem, recv_sem=recv_sem,
            device_id={"tm": device}, device_id_type=MESH,
        )

    def every_chip(act):
        def step(j, carry):
            for i in range(1, rings + 1):
                act(lax.rem(row + i, rings) * side + lax.rem(col + 1 + j, side))
            return carry

        lax.fori_loop(0, side - 1, step, 0)
        for i in range(1, rings):
            act(lax.rem(row + i, rings) * side + col)

    barrier = pltpu.get_barrier_semaphore()

    @pl.when(me > 0)
    def _():
        signal(barrier, me - 1)

    @pl.when(me > 1)
    def _():
        signal(barrier, 0)

    early = frames - hist
    loads = [
        pltpu.make_async_copy(
            volt.at[p, pl.ds(begin, size)], x.at[p, pl.ds(hist + begin, size)], load_sem.at[2 * k + p]
        )
        for k, (begin, size) in enumerate([(early, hist), (0, early)])
        for p in range(2)
    ]
    for k, (source, target) in enumerate(
        [(coef, c), (first, b1), (twist, tw), (second, b2), (delays, dl), (mask, mk)]
    ):
        loads.append(pltpu.make_async_copy(source, target, load_sem.at[4 + k]))
    for load in loads:
        load.start()

    def halo(k):
        p, rows = k // 2, pl.ds((k % 2) * 16, 16)
        return send(
            x.at[p, pl.ds(frames, hist), rows], x.at[p, pl.ds(0, hist), rows],
            halo_send.at[k], halo_recv.at[k], me + 1,
        )

    @pl.when(me == 0)
    def _():
        pl.semaphore_wait(barrier, last)
        signal(go_sem, 1)

    loads[0].wait()
    loads[1].wait()

    @pl.when((me > 0) & (me < last))
    def _():
        pl.semaphore_wait(barrier, 1)

    @pl.when(me < last)
    def _():
        for k in range(4):
            halo(k).start()

    @pl.when(me == 0)
    def _():
        x[:, :hist] = jnp.zeros((2, hist, 2 * LOW, HIGH), BF16)

    for load in loads[2:]:
        load.wait()

    def weigh(block, k):
        p, r = k // 2, lax.rem(k, 2)
        rows = pl.ds(pl.multiple_of(r * 16, 16), 16)
        lanes = pl.ds(pl.multiple_of(p * LANES, LANES), LANES)
        sums = [None] * BLOCK
        for i in range(BLOCK + hist):
            value = x[p, block * BLOCK + i, rows, :].astype(F32)
            for f in range(BLOCK):
                tap = i - f
                if 0 <= tap < TAPS:
                    term = c[tap, rows, :] * value
                    sums[f] = term if tap == 0 else sums[f] + term
                    if tap == TAPS - 1:
                        high = sums[f].astype(BF16)
                        low = (sums[f] - high.astype(F32)).astype(BF16)
                        spot = pl.ds(pl.multiple_of(f * 32 + r * 16, 16), 16)
                        wh[block, spot, lanes] = high
                        wl[block, spot, lanes] = low

    def transform(pair):
        half = LOW * BLOCK
        energies = []
        turns = [
            dot(b1[0], wh[b]) + dot(b1[0], wl[b]) + dot(b1[1], wh[b]) for b in (2 * pair, 2 * pair + 1)
        ]
        for z in turns:
            energy = None
            for p in range(2):
                zr = z[:half, p * LANES : (p + 1) * LANES]
                zi = z[half:, p * LANES : (p + 1) * LANES]
                turned = jnp.concatenate([zr * tw[0] + zi * tw[1], zi * tw[0] - zr * tw[1]], axis=1)
                high = turned.astype(BF16)
                low = (turned - high.astype(F32)).astype(BF16)
                u = dot(high, b2[0]) + dot(high, b2[1]) + dot(low, b2[0])
                power = u[:, :HIGH] * u[:, :HIGH] + u[:, HIGH:] * u[:, HIGH:]
                energy = power if p == 0 else energy + power
            energies.append(energy)
        for k in range(LOW):
            both = jnp.concatenate([e[k * BLOCK : (k + 1) * BLOCK] for e in energies], axis=0)
            det[2 * pair * BLOCK : 2 * (pair + 1) * BLOCK, k * HIGH : (k + 1) * HIGH] = both.astype(BF16)

    def late_half(k, carry):
        weigh(2, k)
        weigh(3, k)
        return carry

    lax.fori_loop(0, 4, late_half, 0)
    transform(1)

    used = jnp.where(mk[...] > 0, dl[...], -1).astype(F32).astype(BF16)
    lane = lax.broadcasted_iota(jnp.int32, (trials, LANES), 1)
    trial = lax.broadcasted_iota(jnp.int32, (trials, LANES), 0)
    spread = (lax.rem(lane, trials) == trial).astype(F32).astype(BF16)
    live = jnp.maximum(jnp.sum(mk[...].astype(F32)), 1.0)
    dt32[...] = lax.dot_general(used, spread, (((0,), (0,)), ((), ())), preferred_element_type=F32)
    lane_k = lax.broadcasted_iota(jnp.int32, (HIGH, LANES), 1)
    offset = (lane_k // trials).astype(F32)
    for k in range(LOW):
        rows = dt32[pl.ds(k, HIGH, stride=LOW), :] - offset
        dtm[k * HIGH : (k + 1) * HIGH, :LANES] = rows.astype(jnp.int32).astype(I16)
        dtm[k * HIGH : (k + 1) * HIGH, LANES:] = (rows - 2.0).astype(jnp.int32).astype(I16)
    acc[...] = jnp.zeros_like(acc)

    span = DSPAN * frames
    chunk = 2 * HIGH
    ahead = frames // 8
    part_rows = frames // 2

    ones = jnp.ones((chunk, 2 * LANES), BF16)
    zeros = jnp.zeros((chunk, 2 * LANES), BF16)

    def chosen(k, base):
        target = jnp.full((chunk, 2 * LANES), base, jnp.int32).astype(I16)
        return jnp.where(dtm[k * chunk : (k + 1) * chunk, :] == target, ones, zeros).astype(F8)

    def select(begin, size, a, h, stored):
        total = None
        for k in range(NCHAN // chunk):
            rows = slice(k * chunk, (k + 1) * chunk)
            weights = sel[2 * a + h, rows, :] if stored else chosen(k, 8 * a + 4 * h)
            term = dot(det[begin : begin + size, rows], weights)
            total = term if k == 0 else total + term
        return total

    def shifts(first_row, size, stored):
        def shift(i, carry):
            totals = []
            for j in range(ahead):
                a = i * ahead + j
                totals.append([select(first_row, size, a, h, stored) for h in range(2)])
            for j in range(ahead):
                begin = pl.multiple_of(span + first_row - 8 * (i * ahead + j), 8)
                for h in range(2):
                    acc[h, pl.ds(begin, size), :] += totals[j][h]
            return carry

        lax.fori_loop(0, jnp.minimum(me + 1, DSPAN), shift, 0)

        @pl.when(me >= DSPAN)
        def _():
            acc[0, first_row : first_row + size, :] += select(first_row, size, span // 8, 0, stored)

    fed_late = (me == 1) | ((me > 1) & (lax.rem(me, CORES * side) == 0))

    @pl.when(fed_late)
    def _():
        def keep(q, carry):
            for k in range(NCHAN // chunk):
                sel[q, k * chunk : (k + 1) * chunk, :] = chosen(k, 4 * q)
            return carry

        lax.fori_loop(0, span // 4 + 1, keep, 0)
        shifts(part_rows, part_rows, True)

    @pl.when(me == 1)
    def _():
        pl.semaphore_wait(go_sem, 1)
        signal(past_sem, 2)
        signal(go_sem, 2)
        signal(go_sem, 3)

    for k in range(4):

        @pl.when(me > 0)
        def _():
            halo(k).wait_recv()

        if k == 0:

            @pl.when((me > 1) & (me < last))
            def _():
                signal(past_sem, me + 1)

        def early_half(block, carry):
            weigh(block, k)
            return carry

        lax.fori_loop(0, 2, early_half, 0)

    transform(0)

    def hear(now):
        @pl.when((me > 1) & now)
        def _():
            pl.semaphore_wait(past_sem, 1)

            @pl.when(me < last)
            def _():
                signal(past2_sem, me + 1)

    top = lax.rem(place, side) == 0
    hear(((core == 0) & (me > 2)) | ((core == 1) & jnp.logical_not(top)))

    @pl.when(fed_late)
    def _():
        shifts(0, part_rows, True)

    @pl.when(jnp.logical_not(fed_late))
    def _():
        shifts(0, frames, False)

    hear(((core == 1) & top) | (me == 2))

    even, odd = None, None
    rows_out = span + frames
    for h in range(2):
        for half in range(2):
            lanes = slice(half * LANES, (half + 1) * LANES)
            first_row = 4 * h + 2 * half
            left = acc[h, first_row : first_row + rows_out, lanes]
            right = acc[h, first_row + 1 : first_row + 1 + rows_out, lanes]
            even = left if even is None else even + left
            odd = right if odd is None else odd + right
    part[...] = even + pltpu.roll(odd, trials, 1)

    def part_copy(k):
        return send(
            part.at[pl.ds(span - k * frames, frames)], parts_in.at[k - 1],
            part_send.at[k - 1], part_recv.at[k - 1], me - k,
        )

    for k in range(1, DSPAN + 1):

        @pl.when(me >= k)
        def _():
            if k == DSPAN:
                pl.semaphore_wait(past2_sem, 1)
            part_copy(k).start()

        @pl.when(me + k > last)
        def _():
            parts_in[k - 1] = jnp.zeros((frames, LANES), F32)

    @pl.when((me == 2) | (me == 3))
    def _():
        pl.semaphore_wait(go_sem, 1)

        def tell(k, carry):
            for j in range(1, SOME + 1):
                signal(all_sem, me + 2 * (k * SOME + j))
            return carry

        others = (tm_size - 4) // 2
        lax.fori_loop(0, others // SOME, tell, 0)
        for j in range(others // SOME * SOME + 1, others + 1):
            signal(all_sem, me + 2 * j)

    for k in range(1, DSPAN + 1):

        @pl.when(me + k <= last)
        def _():
            part_copy(k).wait_recv()

    series = part[span:, :]
    for k in range(DSPAN):
        series = series + parts_in[k]

    def pack(mean, second, peak):
        wide = lax.broadcasted_iota(jnp.int32, (1, LANES), 1)
        head = jnp.where(wide < trials, mean, pltpu.roll(second, trials, 1))
        return jnp.concatenate([head, peak], axis=0)

    def merge(slots, steps, count):
        entries = slots[...]
        mean = jnp.sum(entries, axis=0) / steps
        away = entries - mean[None]
        spread_sum = jnp.sum(away * away, axis=0)
        second = pltpu.roll(mean * steps, trials, 1) + count * spread_sum
        return mean[0:1], second[0:1], jnp.max(entries, axis=0)[1:2]

    mean = jnp.sum(series, axis=0, keepdims=True) / frames
    away = series - mean
    second_sum = jnp.sum(away * away, axis=0, keepdims=True)
    st_a[0] = pack(mean, second_sum, jnp.max(series, axis=0, keepdims=True))
    part[span:, :] = series

    @pl.when(me > 3)
    def _():
        pl.semaphore_wait(all_sem, 1)

    pair = send(st_a.at[0], st_a.at[1], pair_send, pair_recv, me + 1 - 2 * core)
    pair.start()
    pair.wait_recv()
    st_b[place] = pack(*merge(st_a, CORES, float(frames)))

    def chip_copy(chip):
        return send(st_b.at[place], st_b.at[place], b_send, b_recv, chip * CORES + core)

    every_chip(lambda chip: chip_copy(chip).start())
    others = st_b.at[pl.ds(0, chips - 1)]
    pltpu.make_async_copy(others, others, b_recv).wait()

    average, second_sum, peak = merge(st_b, chips, float(frames * CORES))
    variance = second_sum / (frames * tm_size)
    deviation = jnp.sqrt(variance + 1e-05)
    zout[...] = ((part[span:, :] - average) / deviation)[:, :trials]
    rows = jnp.concatenate([average / live, deviation / live, (peak - average) / deviation], axis=0)
    stats_out[...] = rows[:, :trials]

    pair.wait_send()
    pltpu.make_async_copy(others, others, b_send).wait()

    @pl.when(me < last)
    def _():
        for k in range(4):
            halo(k).wait_send()

    for k in range(1, DSPAN + 1):

        @pl.when(me >= k)
        def _():
            part_copy(k).wait_send()


def per_device(tm_size, voltage, delays, chan_mask):
    frames = voltage.shape[2] // NCHAN
    trials = delays.shape[0]
    rows = voltage.shape[2] // HIGH
    volt = voltage.reshape(2, 2, rows, HIGH).transpose(0, 2, 1, 3).reshape(2, frames, 2 * LOW, HIGH)
    hist = TAPS - 1
    side = 2 * LOW * BLOCK
    vmem = pltpu.VMEM
    dma = pltpu.SemaphoreType.DMA
    span = DSPAN * frames
    zscore, stats = pl.pallas_call(
        functools.partial(kernel, tm_size, frames, trials),
        out_shape=(
            jax.ShapeDtypeStruct((frames, trials), F32),
            jax.ShapeDtypeStruct((3, trials), F32),
        ),
        in_specs=[pl.BlockSpec(memory_space=pl.ANY)] * 7,
        out_specs=(pl.BlockSpec(memory_space=pltpu.VMEM),) * 2,
        scratch_shapes=[
            vmem((2, hist + frames, 2 * LOW, HIGH), BF16),
            vmem((TAPS, 2 * LOW, HIGH), F32),
            vmem((2, side, side), BF16),
            vmem((2, LOW * BLOCK, HIGH), F32),
            vmem((2, 2 * HIGH, 2 * HIGH), BF16),
            vmem((trials, NCHAN), jnp.int32),
            vmem((1, NCHAN), jnp.int32),
            vmem((frames // BLOCK, side, 2 * LANES), BF16),
            vmem((frames // BLOCK, side, 2 * LANES), BF16),
            vmem((frames, NCHAN), BF16),
            vmem((NCHAN, LANES), F32),
            vmem((NCHAN, 2 * LANES), I16),
            vmem((span // 4 + 1, NCHAN, 2 * LANES), F8),
            vmem((2, span + frames + 8, 2 * LANES), F32),
            vmem((span + frames, LANES), F32),
            vmem((DSPAN, frames, LANES), F32),
            vmem((CORES, 2, LANES), F32),
            vmem((tm_size // CORES, 2, LANES), F32),
            dma((10,)),
            pltpu.SemaphoreType.REGULAR,
            pltpu.SemaphoreType.REGULAR,
            pltpu.SemaphoreType.REGULAR,
            pltpu.SemaphoreType.REGULAR,
            dma((4,)),
            dma((4,)),
            dma((DSPAN,)),
            dma((DSPAN,)),
            dma,
            dma,
            dma,
            dma,
        ],
        compiler_params=pltpu.CompilerParams(
            collective_id=0, has_side_effects=True, vmem_limit_bytes=40 << 20
        ),
    )(
        *(
            pltpu.with_memory_space_constraint(value, pltpu.HBM)
            for value in (
                volt, delays, chan_mask.reshape(1, NCHAN),
                jnp.asarray(filter_table()), jnp.asarray(first_table()),
                jnp.asarray(twist_table()), jnp.asarray(second_table()),
            )
        )
    )
    zscore, stats = pl.pallas_call(
        hand_on,
        out_shape=(
            jax.ShapeDtypeStruct((frames, trials), F32),
            jax.ShapeDtypeStruct((3, trials), F32),
        ),
        in_specs=[pl.BlockSpec(memory_space=pltpu.VMEM)] * 2,
        out_specs=(pl.BlockSpec(memory_space=pl.ANY),) * 2,
        scratch_shapes=[dma((2,))],
        compiler_params=pltpu.CompilerParams(vmem_limit_bytes=1 << 20),
    )(zscore, stats)
    return zscore.T, stats


def solution(mesh):
    return jax.shard_map(
        functools.partial(per_device, mesh.shape["tm"]),
        mesh=mesh,
        in_specs=(P(None, None, ("beam", "tm")), P(), P("beam")),
        out_specs=(P(None, ("beam", "tm")), P(None, "beam")),
        check_vma=False,
    )
```

```python
import functools

import jax
import jax.numpy as jnp
import numpy as np
from jax import lax
from jax.experimental import pallas as pl
from jax.experimental.pallas import tpu as pltpu
from jax.sharding import PartitionSpec as P

NCHAN = 2048
TAPS = 16
LOW = 16
HIGH = 128
BLOCK = 8
GROUP = 16
LANES = 128
DSPAN = 3
CORES = 2
SOME = 9
MESH = pl.DeviceIdType.MESH
F32 = jnp.float32
BF16 = jnp.bfloat16
I8 = jnp.int8
F8 = jnp.float8_e4m3fn


def filter_table():
    length = TAPS * NCHAN
    position = np.arange(length, dtype=np.float64)
    centred = (position - (length - 1) / 2.0) / NCHAN
    window = 0.54 - 0.46 * np.cos(2.0 * np.pi * position / (length - 1))
    shaped = np.sinc(centred) * window
    shaped = shaped * np.sqrt(NCHAN / np.sum(shaped * shaped))
    rows = shaped.reshape(TAPS, LOW, 1, HIGH)
    return np.broadcast_to(rows, (TAPS, LOW, 2, HIGH)).reshape(TAPS, 2 * LOW, HIGH).astype(np.float32)


def split_table(table):
    high = table.astype(np.float32).astype(jnp.bfloat16)
    low = (table - high.astype(np.float64)).astype(np.float32).astype(jnp.bfloat16)
    return np.stack([high, low])


def first_table():
    angle = 2.0 * np.pi * (np.outer(np.arange(LOW), np.arange(LOW)) % LOW) / LOW
    turn = np.empty((2, LOW, LOW, 2))
    turn[0, :, :, 0] = np.cos(angle)
    turn[0, :, :, 1] = np.sin(angle)
    turn[1, :, :, 0] = -np.sin(angle)
    turn[1, :, :, 1] = np.cos(angle)
    full = np.zeros((2, LOW, BLOCK, BLOCK, LOW, 2))
    for frame in range(BLOCK):
        full[:, :, frame, frame] = turn
    side = 2 * LOW * BLOCK
    return split_table(full.reshape(side, side))


def twist_table():
    angle = 2.0 * np.pi * np.outer(np.arange(LOW), np.arange(HIGH)) / NCHAN
    both = np.stack([np.cos(angle), np.sin(angle)])
    return np.repeat(both, BLOCK, axis=1).astype(np.float32)


def second_table():
    angle = 2.0 * np.pi * (np.outer(np.arange(HIGH), np.arange(HIGH)) % HIGH) / HIGH
    top = np.concatenate([np.cos(angle), -np.sin(angle)], axis=1)
    bottom = np.concatenate([np.sin(angle), np.cos(angle)], axis=1)
    return split_table(np.concatenate([top, bottom], axis=0) / np.sqrt(NCHAN))


def dot(a, b):
    return lax.dot_general(a, b, (((1,), (0,)), ((), ())), preferred_element_type=F32)


def hand_on(zscore, stats, zout, stats_out, sems):
    copies = [pltpu.make_async_copy(zscore, zout, sems.at[0]), pltpu.make_async_copy(stats, stats_out, sems.at[1])]
    for copy in copies:
        copy.start()
    for copy in copies:
        copy.wait()


def kernel(
    tm_size, frames, trials,
    volt, delays, mask, coef, first, twist, second,
    zout, stats_out,
    x, c, b1, tw, b2, dl, mk, wh, wl, det, dt32, dtm, acc, part, parts_in, st_a, st_b,
    load_sem, go_sem, all_sem, past_sem, past2_sem, halo_send, halo_recv, part_send, part_recv, pair_send, pair_recv,
    b_send, b_recv,
):
    me = lax.axis_index("tm")
    hist = TAPS - 1
    last = tm_size - 1
    rings = tm_size // GROUP
    side = GROUP // CORES
    core = lax.rem(me, CORES)
    place = me // CORES
    row, col = place // side, lax.rem(place, side)
    chips = rings * side

    def signal(sem, target):
        pl.semaphore_signal(sem, inc=1, device_id={"tm": target}, device_id_type=MESH)

    def send(source, target, send_sem, recv_sem, device):
        return pltpu.make_async_remote_copy(
            src_ref=source, dst_ref=target, send_sem=send_sem, recv_sem=recv_sem,
            device_id={"tm": device}, device_id_type=MESH,
        )

    def every_chip(act):
        def step(j, carry):
            for i in range(1, rings + 1):
                act(lax.rem(row + i, rings) * side + lax.rem(col + 1 + j, side))
            return carry

        lax.fori_loop(0, side - 1, step, 0)
        for i in range(1, rings):
            act(lax.rem(row + i, rings) * side + col)

    barrier = pltpu.get_barrier_semaphore()

    @pl.when(me > 0)
    def _():
        signal(barrier, me - 1)

    @pl.when(me > 1)
    def _():
        signal(barrier, 0)

    early = frames - hist
    loads = [
        pltpu.make_async_copy(
            volt.at[p, pl.ds(begin, size)], x.at[p, pl.ds(hist + begin, size)], load_sem.at[2 * k + p]
        )
        for k, (begin, size) in enumerate([(early, hist), (0, early)])
        for p in range(2)
    ]
    for k, (source, target) in enumerate(
        [(coef, c), (first, b1), (twist, tw), (second, b2), (delays, dl), (mask, mk)]
    ):
        loads.append(pltpu.make_async_copy(source, target, load_sem.at[4 + k]))
    for load in loads:
        load.start()

    def halo(k):
        p, rows = k // 2, pl.ds((k % 2) * 16, 16)
        return send(
            x.at[p, pl.ds(frames, hist), rows], x.at[p, pl.ds(0, hist), rows],
            halo_send.at[k], halo_recv.at[k], me + 1,
        )

    @pl.when(me == 0)
    def _():
        pl.semaphore_wait(barrier, last)
        signal(go_sem, 1)

    loads[0].wait()
    loads[1].wait()

    @pl.when((me > 0) & (me < last))
    def _():
        pl.semaphore_wait(barrier, 1)

    @pl.when(me < last)
    def _():
        for k in range(4):
            halo(k).start()

    @pl.when(me == 0)
    def _():
        x[:, :hist] = jnp.zeros((2, hist, 2 * LOW, HIGH), BF16)

    for load in loads[2:5]:
        load.wait()

    def weigh(block, k):
        p, r = k // 2, lax.rem(k, 2)
        rows = pl.ds(pl.multiple_of(r * 16, 16), 16)
        lanes = pl.ds(pl.multiple_of(p * LANES, LANES), LANES)
        sums = [None] * BLOCK
        for i in range(BLOCK + hist):
            value = x[p, block * BLOCK + i, rows, :].astype(F32)
            for f in range(BLOCK):
                tap = i - f
                if 0 <= tap < TAPS:
                    term = c[tap, rows, :] * value
                    sums[f] = term if tap == 0 else sums[f] + term
                    if tap == TAPS - 1:
                        high = sums[f].astype(BF16)
                        low = (sums[f] - high.astype(F32)).astype(BF16)
                        spot = pl.ds(pl.multiple_of(f * 32 + r * 16, 16), 16)
                        wh[block, spot, lanes] = high
                        wl[block, spot, lanes] = low

    def transform(pair):
        half = LOW * BLOCK
        energies = []
        turns = [
            dot(b1[0], wh[b]) + dot(b1[0], wl[b]) + dot(b1[1], wh[b]) for b in (2 * pair, 2 * pair + 1)
        ]
        for z in turns:
            energy = None
            for p in range(2):
                zr = z[:half, p * LANES : (p + 1) * LANES]
                zi = z[half:, p * LANES : (p + 1) * LANES]
                turned = jnp.concatenate([zr * tw[0] + zi * tw[1], zi * tw[0] - zr * tw[1]], axis=1)
                high = turned.astype(BF16)
                low = (turned - high.astype(F32)).astype(BF16)
                u = dot(high, b2[0]) + dot(high, b2[1]) + dot(low, b2[0])
                power = u[:, :HIGH] * u[:, :HIGH] + u[:, HIGH:] * u[:, HIGH:]
                energy = power if p == 0 else energy + power
            energies.append(energy)
        for k in range(LOW):
            both = jnp.concatenate([e[k * BLOCK : (k + 1) * BLOCK] for e in energies], axis=0)
            det[2 * pair * BLOCK : 2 * (pair + 1) * BLOCK, k * HIGH : (k + 1) * HIGH] = both.astype(BF16)

    def late_half(k, carry):
        weigh(2, k)
        weigh(3, k)
        return carry

    lax.fori_loop(0, 4, late_half, 0)
    for load in loads[5:8]:
        load.wait()
    transform(1)

    for load in loads[8:]:
        load.wait()

    used = jnp.where(mk[...] > 0, dl[...], -1).astype(F32).astype(BF16)
    lane = lax.broadcasted_iota(jnp.int32, (trials, LANES), 1)
    trial = lax.broadcasted_iota(jnp.int32, (trials, LANES), 0)
    spread = (lax.rem(lane, trials) == trial).astype(F32).astype(BF16)
    live = jnp.maximum(jnp.sum(mk[...].astype(F32)), 1.0)
    dt32[...] = lax.dot_general(used, spread, (((0,), (0,)), ((), ())), preferred_element_type=F32)
    lane_k = lax.broadcasted_iota(jnp.int32, (HIGH, LANES), 1)
    offset = (lane_k // trials).astype(F32)
    for k in range(LOW):
        rows = dt32[pl.ds(k, HIGH, stride=LOW), :] - offset
        dtm[k * HIGH : (k + 1) * HIGH, :LANES] = rows.astype(jnp.int32).astype(I8)
        dtm[k * HIGH : (k + 1) * HIGH, LANES:] = (rows - 2.0).astype(jnp.int32).astype(I8)
    acc[...] = jnp.zeros_like(acc)

    @pl.when(me == 1)
    def _():
        pl.semaphore_wait(go_sem, 1)
        signal(past_sem, 2)
        signal(go_sem, 2)
        signal(go_sem, 3)

    for k in range(4):

        @pl.when(me > 0)
        def _():
            halo(k).wait_recv()

        if k == 0:

            @pl.when((me > 1) & (me < last))
            def _():
                signal(past_sem, me + 1)

        def early_half(block, carry):
            weigh(block, k)
            return carry

        lax.fori_loop(0, 2, early_half, 0)

    transform(0)

    def hear(now):
        @pl.when((me > 1) & now)
        def _():
            pl.semaphore_wait(past_sem, 1)

            @pl.when(me < last)
            def _():
                signal(past2_sem, me + 1)

    top = lax.rem(place, side) == 0
    hear(((core == 0) & (me > 2)) | ((core == 1) & jnp.logical_not(top)))

    span = DSPAN * frames
    chunk = 2 * HIGH
    ahead = frames // 8

    ones = jnp.ones((chunk, 2 * LANES), F8)
    zeros = jnp.zeros((chunk, 2 * LANES), F8)

    def select(base):
        target = jnp.full((chunk, 2 * LANES), base, jnp.int32).astype(I8)
        total = None
        for k in range(NCHAN // chunk):
            rows = slice(k * chunk, (k + 1) * chunk)
            term = dot(det[:, rows], jnp.where(dtm[rows, :] == target, ones, zeros))
            total = term if k == 0 else total + term
        return total

    def shift(i, carry):
        totals = [[select(8 * (i * ahead + j) + 4 * h) for h in range(2)] for j in range(ahead)]
        for j in range(ahead):
            begin = pl.multiple_of(span - 8 * (i * ahead + j), 8)
            for h in range(2):
                acc[h, pl.ds(begin, frames), :] += totals[j][h]
        return carry

    lax.fori_loop(0, jnp.minimum(me + 1, DSPAN), shift, 0)

    @pl.when(me >= DSPAN)
    def _():
        acc[0, 0:frames, :] += select(span)

    hear(((core == 1) & top) | (me == 2))

    even, odd = None, None
    rows_out = span + frames
    for h in range(2):
        for half in range(2):
            lanes = slice(half * LANES, (half + 1) * LANES)
            first_row = 4 * h + 2 * half
            left = acc[h, first_row : first_row + rows_out, lanes]
            right = acc[h, first_row + 1 : first_row + 1 + rows_out, lanes]
            even = left if even is None else even + left
            odd = right if odd is None else odd + right
    part[...] = even + pltpu.roll(odd, trials, 1)

    def part_copy(k):
        return send(
            part.at[pl.ds(span - k * frames, frames)], parts_in.at[k - 1],
            part_send.at[k - 1], part_recv.at[k - 1], me - k,
        )

    for k in range(1, DSPAN + 1):

        @pl.when(me >= k)
        def _():
            if k == DSPAN:
                pl.semaphore_wait(past2_sem, 1)
            part_copy(k).start()

        @pl.when(me + k > last)
        def _():
            parts_in[k - 1] = jnp.zeros((frames, LANES), F32)

    @pl.when((me == 2) | (me == 3))
    def _():
        pl.semaphore_wait(go_sem, 1)

        def tell(k, carry):
            for j in range(1, SOME + 1):
                signal(all_sem, me + 2 * (k * SOME + j))
            return carry

        others = (tm_size - 4) // 2
        lax.fori_loop(0, others // SOME, tell, 0)
        for j in range(others // SOME * SOME + 1, others + 1):
            signal(all_sem, me + 2 * j)

    for k in range(1, DSPAN + 1):

        @pl.when(me + k <= last)
        def _():
            part_copy(k).wait_recv()

    series = part[span:, :]
    for k in range(DSPAN):
        series = series + parts_in[k]

    def pack(mean, second, peak):
        wide = lax.broadcasted_iota(jnp.int32, (1, LANES), 1)
        head = jnp.where(wide < trials, mean, pltpu.roll(second, trials, 1))
        return jnp.concatenate([head, peak], axis=0)

    def merge(slots, steps, count):
        entries = slots[...]
        mean = jnp.sum(entries, axis=0) / steps
        away = entries - mean[None]
        spread_sum = jnp.sum(away * away, axis=0)
        second = pltpu.roll(mean * steps, trials, 1) + count * spread_sum
        return mean[0:1], second[0:1], jnp.max(entries, axis=0)[1:2]

    mean = jnp.sum(series, axis=0, keepdims=True) / frames
    away = series - mean
    second_sum = jnp.sum(away * away, axis=0, keepdims=True)
    st_a[0] = pack(mean, second_sum, jnp.max(series, axis=0, keepdims=True))
    part[span:, :] = series

    pair = send(st_a.at[0], st_a.at[1], pair_send, pair_recv, me + 1 - 2 * core)
    pair.start()
    pair.wait_recv()
    st_b[place] = pack(*merge(st_a, CORES, float(frames)))

    @pl.when(me > 3)
    def _():
        pl.semaphore_wait(all_sem, 1)

    def chip_copy(chip):
        return send(st_b.at[place], st_b.at[place], b_send, b_recv, chip * CORES + core)

    every_chip(lambda chip: chip_copy(chip).start())
    others = st_b.at[pl.ds(0, chips - 1)]
    pltpu.make_async_copy(others, others, b_recv).wait()

    average, second_sum, peak = merge(st_b, chips, float(frames * CORES))
    variance = second_sum / (frames * tm_size)
    deviation = jnp.sqrt(variance + 1e-05)
    zout[...] = ((part[span:, :] - average) / deviation)[:, :trials]
    rows = jnp.concatenate([average / live, deviation / live, (peak - average) / deviation], axis=0)
    stats_out[...] = rows[:, :trials]

    pair.wait_send()
    pltpu.make_async_copy(others, others, b_send).wait()

    @pl.when(me < last)
    def _():
        for k in range(4):
            halo(k).wait_send()

    for k in range(1, DSPAN + 1):

        @pl.when(me >= k)
        def _():
            part_copy(k).wait_send()


def per_device(tm_size, voltage, delays, chan_mask):
    frames = voltage.shape[2] // NCHAN
    trials = delays.shape[0]
    rows = voltage.shape[2] // HIGH
    volt = voltage.reshape(2, 2, rows, HIGH).transpose(0, 2, 1, 3).reshape(2, frames, 2 * LOW, HIGH)
    hist = TAPS - 1
    side = 2 * LOW * BLOCK
    vmem = pltpu.VMEM
    dma = pltpu.SemaphoreType.DMA
    span = DSPAN * frames
    zscore, stats = pl.pallas_call(
        functools.partial(kernel, tm_size, frames, trials),
        out_shape=(
            jax.ShapeDtypeStruct((frames, trials), F32),
            jax.ShapeDtypeStruct((3, trials), F32),
        ),
        in_specs=[pl.BlockSpec(memory_space=pl.ANY)] * 7,
        out_specs=(pl.BlockSpec(memory_space=pltpu.VMEM),) * 2,
        scratch_shapes=[
            vmem((2, hist + frames, 2 * LOW, HIGH), BF16),
            vmem((TAPS, 2 * LOW, HIGH), F32),
            vmem((2, side, side), BF16),
            vmem((2, LOW * BLOCK, HIGH), F32),
            vmem((2, 2 * HIGH, 2 * HIGH), BF16),
            vmem((trials, NCHAN), jnp.int32),
            vmem((1, NCHAN), jnp.int32),
            vmem((frames // BLOCK, side, 2 * LANES), BF16),
            vmem((frames // BLOCK, side, 2 * LANES), BF16),
            vmem((frames, NCHAN), BF16),
            vmem((NCHAN, LANES), F32),
            vmem((NCHAN, 2 * LANES), I8),
            vmem((2, span + frames + 8, 2 * LANES), F32),
            vmem((span + frames, LANES), F32),
            vmem((DSPAN, frames, LANES), F32),
            vmem((CORES, 2, LANES), F32),
            vmem((tm_size // CORES, 2, LANES), F32),
            dma((10,)),
            pltpu.SemaphoreType.REGULAR,
            pltpu.SemaphoreType.REGULAR,
            pltpu.SemaphoreType.REGULAR,
            pltpu.SemaphoreType.REGULAR,
            dma((4,)),
            dma((4,)),
            dma((DSPAN,)),
            dma((DSPAN,)),
            dma,
            dma,
            dma,
            dma,
        ],
        compiler_params=pltpu.CompilerParams(
            collective_id=0, has_side_effects=True, vmem_limit_bytes=40 << 20
        ),
    )(
        *(
            pltpu.with_memory_space_constraint(value, pltpu.HBM)
            for value in (
                volt, delays, chan_mask.reshape(1, NCHAN),
                jnp.asarray(filter_table()), jnp.asarray(first_table()),
                jnp.asarray(twist_table()), jnp.asarray(second_table()),
            )
        )
    )
    zscore, stats = pl.pallas_call(
        hand_on,
        out_shape=(
            jax.ShapeDtypeStruct((frames, trials), F32),
            jax.ShapeDtypeStruct((3, trials), F32),
        ),
        in_specs=[pl.BlockSpec(memory_space=pltpu.VMEM)] * 2,
        out_specs=(pl.BlockSpec(memory_space=pl.ANY),) * 2,
        scratch_shapes=[dma((2,))],
        compiler_params=pltpu.CompilerParams(vmem_limit_bytes=1 << 20),
    )(zscore, stats)
    return zscore.T, stats


def solution(mesh):
    return jax.shard_map(
        functools.partial(per_device, mesh.shape["tm"]),
        mesh=mesh,
        in_specs=(P(None, None, ("beam", "tm")), P(), P("beam")),
        out_specs=(P(None, ("beam", "tm")), P(None, "beam")),
        check_vma=False,
    )
```
